16 devices in a mesh: dp: 16 (over z, y, x, core).
Axes of the slice: x: 2, y: 2, z: 2, core: 2. Of those that a mesh axis runs over, the one named last changes fastest.
Arguments:
- grad_rows: bfloat16 [16, 14147584], P('dp')
- master: float32 [14147584], P('dp')
- mom_first: float32 [14147584], P('dp')
- mom_second: float32 [14147584], P('dp')
- decay_mask: int32 [14147584], P('dp')
- learn_rate: float32 [1], replicated
Outputs:
- output 1: bfloat16 [14147584], replicated
- output 2: float32 [14147584], P('dp')
- output 3: float32 [14147584], P('dp')
- output 4: float32 [14147584], P('dp')
- output 5: float32 [1], replicated
All inputs are finite; a program needn't handle non-finite values.
Results may differ from the reference program's by a relative error of at most 0.001.
Values are sent between devices in bfloat16 or wider.
A program may use at most 1 GiB of HBM per device.

```python
import jax
import jax.numpy as jnp
from jax import lax

NUM_DEV = 16
MODEL_WIDTH = 800
MLP_HIDDEN = 2160
VOCAB_ROWS = 8000
PADDED = 14147584
ADAM_STEP = 10

BETA_FIRST = 0.9
BETA_SECOND = 0.95
ADAM_EPS = 1e-8
CLIP_EPS = 1e-6
WEIGHT_DECAY = 0.1


def decay_layout(mask_key):
    seg_lens = [VOCAB_ROWS * MODEL_WIDTH, MODEL_WIDTH * MODEL_WIDTH, MODEL_WIDTH * MODEL_WIDTH, MODEL_WIDTH * MODEL_WIDTH, MODEL_WIDTH * MODEL_WIDTH, MODEL_WIDTH * MLP_HIDDEN, MODEL_WIDTH * MLP_HIDDEN, MLP_HIDDEN * MODEL_WIDTH, MODEL_WIDTH, MODEL_WIDTH, MODEL_WIDTH, MODEL_WIDTH]
    seg_flags = [0, 1, 1, 1, 1, 1, 1, 1, 0, 0, 0, 0]
    tensor_order = jax.random.permutation(mask_key, len(seg_lens))
    lens_perm = jnp.array(seg_lens, dtype=jnp.int32)[tensor_order]
    flags_perm = jnp.concatenate([jnp.array(seg_flags, dtype=jnp.int32)[tensor_order], jnp.zeros((1,), jnp.int32)])
    seg_ends = jnp.cumsum(lens_perm)
    seg_pos = jnp.searchsorted(seg_ends, jnp.arange(PADDED, dtype=jnp.int32), side='right')
    return flags_perm[seg_pos]


def setup_inputs(seed: int = 0) -> dict:
    key_list = jax.random.split(jax.random.key(seed), 8)
    dev_scale = 2.0 ** jax.random.uniform(key_list[0], (NUM_DEV,), jnp.float32, -1.5, 1.5)
    norm_aim = jax.random.uniform(key_list[1], (), jnp.float32, 3.0, 8.0)
    grad_scale = norm_aim * NUM_DEV / jnp.sqrt(jnp.sum(dev_scale * dev_scale) * PADDED)
    row_keys = jax.random.split(key_list[2], NUM_DEV)

    def draw_row(row_args):
        row_key, row_scale = row_args
        row_vals = jax.random.normal(row_key, (PADDED,), jnp.float32) * (grad_scale * row_scale)
        return row_vals.astype(jnp.bfloat16)

    grad_rows = lax.map(draw_row, (row_keys, dev_scale))
    unit_scale = PADDED ** -0.5
    master = jax.random.normal(key_list[3], (PADDED,), jnp.float32)
    mom_first = 0.15 * unit_scale * jax.random.normal(key_list[4], (PADDED,), jnp.float32)
    mom_second = 0.05 * unit_scale * unit_scale * (0.5 + jax.random.uniform(key_list[5], (PADDED,), jnp.float32))
    decay_mask = decay_layout(key_list[6])
    learn_rate = jax.random.uniform(key_list[7], (1,), jnp.float32, 0.5, 1.0)
    return {'grad_rows': grad_rows, 'master': master, 'mom_first': mom_first, 'mom_second': mom_second, 'decay_mask': decay_mask, 'learn_rate': learn_rate}


def reference(grad_rows, master, mom_first, mom_second, decay_mask, learn_rate):
    grad_mean = jnp.sum(grad_rows, axis=0, dtype=jnp.float32) / NUM_DEV
    grad_norm = jnp.sqrt(jnp.sum(grad_mean * grad_mean))
    clip_coef = jnp.minimum(1.0, 1.0 / (grad_norm + CLIP_EPS))
    clipped = grad_mean * clip_coef
    new_first = BETA_FIRST * mom_first + (1.0 - BETA_FIRST) * clipped
    new_second = BETA_SECOND * mom_second + (1.0 - BETA_SECOND) * clipped * clipped
    step_dir = (new_first / (1.0 - BETA_FIRST ** ADAM_STEP)) / (jnp.sqrt(new_second / (1.0 - BETA_SECOND ** ADAM_STEP)) + ADAM_EPS)
    decay_flag = decay_mask.astype(jnp.float32)
    new_master = master - learn_rate[0] * (step_dir + WEIGHT_DECAY * decay_flag * master)
    params = new_master.astype(jnp.bfloat16)
    return params, new_master, new_first, new_second, grad_norm.reshape(1)
```

```python
import jax
import jax.numpy as jnp
from jax import lax
from jax.experimental import pallas as pl
from jax.experimental.pallas import tpu as pltpu
from jax.sharding import PartitionSpec as P

BETA_FIRST = 0.9
BETA_SECOND = 0.95
ADAM_EPS = 1e-8
CLIP_EPS = 1e-6
WEIGHT_DECAY = 0.1
ADAM_STEP = 10

NDEV = 16
LANES = 128
ROWS = 6908
ROWS_PAD = 6912
CHUNKS = 12
CR = 576
CW = CR * LANES
SLAB = 72
NSLAB = CR // SLAB
DEPTH = 4
UNITS = ROWS // 4
PART_UNIT0 = (0, 576, 1152)
PART_COUNT = (4, 4, 5)
PART_UNITS = (144, 144, 115)
PART_BASE = (0, 4, 8)
AG_CHUNKS = 13

MESH = pl.DeviceIdType.MESH


def weight(axis):
    return 2 + axis + axis * axis


def step_of(me, axis):
    w = weight(axis)
    return (1 - 2 * ((me // w) % 2)) * w


def chunk_row(q):
    return CR * q - 4 * (q // (CHUNKS - 1))


def remote(src, dst, ssem, rsem, dev):
    return pltpu.make_async_remote_copy(src_ref=src, dst_ref=dst, send_sem=ssem, recv_sem=rsem, device_id=(dev,), device_id_type=MESH)


def rs_kernel(grad, gout, parts_out, prow, own, par, sb, r1, r2, r3, acc, nrm, psend, precv, s1s, s1r, s2s, s2r, s3s, s3r, ns, nr, lo, lp):
    me = lax.axis_index('dp')
    core = me % 2
    partner = me + 1 - 2 * core

    barrier = pltpu.get_barrier_semaphore()

    def greet(i, _):
        other = lax.rem(me + i, NDEV)
        pl.semaphore_signal(barrier, inc=1, device_id=(other,), device_id_type=MESH)
        return 0

    lax.fori_loop(1, NDEV, greet, 0)
    pl.semaphore_wait(barrier, NDEV - 1)

    def decode(phase, t):
        p = t % 3
        j = t // 3
        if phase == 1:
            o1, o2, o3, k = 1, j % 2, (j // 2) % 2, j // 4
        elif phase == 2:
            o1, o2, o3, k = 0, 1, j % 2, j // 2
        elif phase == 3:
            o1, o2, o3, k = 0, 0, 1, j
        else:
            o1, o2, o3, k = 0, 0, 0, j
        a1, a2, a3 = p, (p + 1) % 3, (p + 2) % 3
        shift = o1 * step_of(me, a1) + o2 * step_of(me, a2) + o3 * step_of(me, a3)
        return p, j, k, a1, a2, a3, shift, 4 * p + k

    base_of = {1: 0, 2: 48, 3: 72, 4: 84}
    count_of = {1: 48, 2: 24, 3: 12, 4: 12}

    def grad_slice(block, q):
        start = pl.multiple_of((block * ROWS + chunk_row(q)) * LANES, LANES)
        return grad.at[:, pl.ds(start, CW)]

    def partner_copy(phase, t):
        _, _, _, _, _, _, shift, q = decode(phase, t)
        s = base_of[phase] + t
        return remote(grad_slice(partner + shift, q), prow.at[s], psend.at[s], precv.at[s], partner)

    for phase in (1, 2, 3, 4):
        def send_rows(t, _, phase=phase):
            partner_copy(phase, t).start()
            return 0
        lax.fori_loop(0, count_of[phase], send_rows, 0)

    def loads(phase, t):
        _, _, _, _, _, _, shift, q = decode(phase, t)
        slot = t % DEPTH
        return (pltpu.make_async_copy(grad_slice(me + shift, q), own.at[slot], lo.at[slot]),
                pltpu.make_async_copy(prow.at[base_of[phase] + t], par.at[slot], lp.at[slot]))

    def start_loads(phase, t):
        partner_copy(phase, t).wait_recv()
        a, b = loads(phase, t)
        a.start()
        b.start()

    def chip_sum(slot, i):
        lo_col = i * SLAB * LANES
        if not isinstance(lo_col, int):
            lo_col = pl.multiple_of(lo_col, SLAB * LANES)
        cols = pl.ds(lo_col, SLAB * LANES)
        v = own[slot, :, cols].astype(jnp.float32) + par[slot, :, cols].astype(jnp.float32)
        return v.reshape(SLAB, LANES)

    def s1_copy(t):
        p, j, k, a1, a2, a3, _, q = decode(1, t)
        return remote(sb.at[t], r1.at[t], s1s.at[t], s1r.at[t], me + step_of(me, a1))

    def r1_at(p, k, o2, o3):
        return ((k * 4) + o3 * 2 + o2) * 3 + p

    def r2_at(p, k, o3):
        return (k * 2 + o3) * 3 + p

    def s2_copy(t):
        p, j, k, a1, a2, a3, _, q = decode(2, t)
        return remote(r1.at[r1_at(p, k, 1, j % 2)], r2.at[t], s2s.at[t], s2r.at[t], me + step_of(me, a2))

    def s3_copy(t):
        p, j, k, a1, a2, a3, _, q = decode(3, t)
        return remote(r2.at[r2_at(p, k, 1)], r3.at[t], s3s.at[t], s3r.at[t], me + step_of(me, a3))

    def run_phase(phase, body, last=None):
        n = count_of[phase]
        for t in range(DEPTH - 1):
            start_loads(phase, t)

        def one(t, _):
            @pl.when(t + DEPTH - 1 < n)
            def _():
                start_loads(phase, t + DEPTH - 1)
            a, b = loads(phase, t)
            a.wait()
            b.wait()
            body(t)
            return 0

        lax.fori_loop(0, n if last is None else n - 1, one, 0)
        if last is not None:
            a, b = loads(phase, n - 1)
            a.wait()
            b.wait()
            last(n - 1)

    def slabs(fn):
        def one(i, _):
            fn(i, pl.ds(pl.multiple_of(i * SLAB, SLAB), SLAB))
            return 0
        lax.fori_loop(0, NSLAB, one, 0)

    def phase1(t):
        slot = t % DEPTH

        def fn(i, rows):
            sb[t, rows, :] = chip_sum(slot, i)
        slabs(fn)
        s1_copy(t).start()

    def phase2(t):
        slot = t % DEPTH
        p, j, k, *_ = decode(2, t)
        src = r1_at(p, k, 1, j % 2)
        s1_copy(src).wait_recv()

        def fn(i, rows):
            r1[src, rows, :] = chip_sum(slot, i) + r1[src, rows, :]
        slabs(fn)
        s2_copy(t).start()

    def phase3(t):
        slot = t % DEPTH
        p, j, k, *_ = decode(3, t)
        s1 = r1_at(p, k, 0, 1)
        s2 = r2_at(p, k, 1)
        s1_copy(s1).wait_recv()
        s2_copy(s2).wait_recv()

        def fn(i, rows):
            r2[s2, rows, :] = chip_sum(slot, i) + r1[s1, rows, :] + r2[s2, rows, :]
        slabs(fn)
        s3_copy(t).start()

    acc[...] = jnp.zeros_like(acc)

    def final_sum(t):
        slot = t % DEPTH
        p, j, k, *_ = decode(4, t)
        s1 = r1_at(p, k, 0, 0)
        s2 = r2_at(p, k, 0)
        s1_copy(s1).wait_recv()
        s2_copy(s2).wait_recv()
        s3_copy(t).wait_recv()

        def value(i, rows):
            v = chip_sum(slot, i) + r1[s1, rows, :] + r2[s2, rows, :] + r3[t, rows, :]
            return v * (1.0 / NDEV)
        return value, 4 * p + k

    def phase4(t):
        value, q = final_sum(t)

        def fn(i, rows):
            v = value(i, rows)
            gout[pl.ds(pl.multiple_of(q * CR + i * SLAB, 8), SLAB), :] = v
            acc[...] += jnp.sum((v * v).reshape(SLAB // 8, 8, LANES), axis=0)
        slabs(fn)

    def phase4_last(t):
        value, _ = final_sum(t)
        start = chunk_row(CHUNKS - 1)
        for i in range(NSLAB):
            v = value(i, pl.ds(i * SLAB, SLAB))
            gout[start + i * SLAB:start + (i + 1) * SLAB, :] = v
            sq = v * v
            if i == 0:
                row = lax.broadcasted_iota(jnp.int32, (SLAB, LANES), 0)
                sq = jnp.where(row < 4, 0.0, sq)
            acc[...] += jnp.sum(sq.reshape(SLAB // 8, 8, LANES), axis=0)

    run_phase(1, phase1)
    run_phase(2, phase2)
    run_phase(3, phase3)
    run_phase(4, phase4, phase4_last)

    nrm[me] = acc[...]

    def norm_copy(i):
        other = lax.rem(me + i, NDEV)
        return remote(acc, nrm.at[me], ns.at[i], nr.at[me], other)

    def norm_arrival(i):
        other = lax.rem(me + i, NDEV)
        return remote(acc, nrm.at[other], ns.at[i], nr.at[other], other)

    def norm_send(i, _):
        norm_copy(i).start()
        return 0

    def norm_wait(i, _):
        norm_arrival(i).wait_recv()
        return 0

    lax.fori_loop(1, NDEV, norm_send, 0)

    def drain(n, copy):
        def one(t, _):
            copy(t).wait_send()
            return 0
        lax.fori_loop(0, n, one, 0)

    for phase in (1, 2, 3, 4):
        drain(count_of[phase], lambda t, phase=phase: partner_copy(phase, t))
    drain(48, s1_copy)
    drain(24, s2_copy)
    drain(12, s3_copy)
    lax.fori_loop(1, NDEV, norm_wait, 0)
    drain(NDEV - 1, lambda t: norm_copy(t + 1))
    total = nrm[0]
    for d in range(1, NDEV):
        total = total + nrm[d]
    parts_out[...] = total


def reduce_scatter(grad):
    f32 = jnp.float32
    dma = pltpu.SemaphoreType.DMA
    return pl.pallas_call(
        rs_kernel,
        out_shape=(jax.ShapeDtypeStruct((ROWS_PAD, LANES), f32), jax.ShapeDtypeStruct((8, LANES), f32), jax.ShapeDtypeStruct((96, 1, CW), jnp.bfloat16)),
        in_specs=[pl.BlockSpec(memory_space=pl.ANY)],
        out_specs=(pl.BlockSpec(memory_space=pltpu.VMEM), pl.BlockSpec(memory_space=pltpu.VMEM), pl.BlockSpec(memory_space=pl.ANY)),
        scratch_shapes=[
            pltpu.VMEM((DEPTH, 1, CW), jnp.bfloat16),
            pltpu.VMEM((DEPTH, 1, CW), jnp.bfloat16),
            pltpu.VMEM((48, CR, LANES), f32),
            pltpu.VMEM((48, CR, LANES), f32),
            pltpu.VMEM((24, CR, LANES), f32),
            pltpu.VMEM((12, CR, LANES), f32),
            pltpu.VMEM((8, LANES), f32),
            pltpu.VMEM((NDEV, 8, LANES), f32),
            dma((96,)), dma((96,)),
            dma((48,)), dma((48,)),
            dma((24,)), dma((24,)),
            dma((12,)), dma((12,)),
            dma((NDEV,)), dma((NDEV,)),
            dma((DEPTH,)), dma((DEPTH,)),
        ],
        compiler_params=pltpu.CompilerParams(collective_id=0, has_side_effects=True, vmem_limit_bytes=56 * 1024 * 1024),
        name='reduce_scatter',
    )(grad)


def adam_kernel(lr, parts, g, w, m, v, mask, p_out, w_out, m_out, v_out, norm_out):
    norm = jnp.sqrt(jnp.sum(parts[...], keepdims=True))
    norm_out[...] = jnp.broadcast_to(norm, norm_out.shape)
    clip = jnp.minimum(1.0, 1.0 / (norm + CLIP_EPS))
    h = g[...] * clip
    m_new = BETA_FIRST * m[...] + (1.0 - BETA_FIRST) * h
    v_new = BETA_SECOND * v[...] + (1.0 - BETA_SECOND) * h * h
    step_dir = (m_new / (1.0 - BETA_FIRST ** ADAM_STEP)) / (jnp.sqrt(v_new / (1.0 - BETA_SECOND ** ADAM_STEP)) + ADAM_EPS)
    old = w[...]
    w_new = old - lr[0] * (step_dir + WEIGHT_DECAY * mask[...].astype(jnp.float32) * old)
    w_out[...] = w_new
    m_out[...] = m_new
    v_out[...] = v_new
    p_out[...] = w_new.astype(jnp.bfloat16)


def adam(lr, parts, g, w, m, v, mask):
    f32 = jnp.float32
    block = pl.BlockSpec((CR, LANES), lambda i: (i, 0))
    whole = pl.BlockSpec((8, LANES), lambda i: (0, 0))
    flat = lambda a: a.reshape(ROWS, LANES)
    state = jax.ShapeDtypeStruct((ROWS, LANES), f32)
    return pl.pallas_call(
        adam_kernel,
        grid=(CHUNKS,),
        out_shape=(jax.ShapeDtypeStruct((ROWS_PAD, LANES), jnp.bfloat16), state, state, state, jax.ShapeDtypeStruct((8, LANES), f32)),
        in_specs=[pl.BlockSpec(memory_space=pltpu.SMEM), whole, block, block, block, block, block],
        out_specs=(block, block, block, block, whole),
        name='adam',
    )(lr, parts, g, flat(w), flat(m), flat(v), flat(mask))


def ag_kernel(mine, out, is_, ir, ds_, dr, lsem):
    me = lax.axis_index('dp')
    partner = me + 1 - 2 * (me % 2)
    barrier = pltpu.get_barrier_semaphore()
    near = [me + step_of(me, a) for a in range(3)]
    for other in near + [partner]:
        pl.semaphore_signal(barrier, inc=1, device_id=(other,), device_id_type=MESH)
    pl.semaphore_wait(barrier, 4)

    def place(p, k, n, dev=me):
        a = [p, (p + 1) % 3, (p + 2) % 3]
        block = dev
        for bit in range(3):
            if (n >> bit) & 1:
                block = block + step_of(me, a[bit])
        return out.at[pl.ds(block * UNITS + PART_UNIT0[p] + PART_UNITS[p] * k, PART_UNITS[p])]

    def source(p, k, n):
        if n == 0:
            return mine.at[pl.ds(PART_UNIT0[p] + PART_UNITS[p] * k, PART_UNITS[p])]
        return place(p, k, n)

    def ici(p, k, hop, n):
        slot = n | (1 << hop)
        c = PART_BASE[p] + k
        return remote(source(p, k, n), place(p, k, n), is_.at[slot, c], ir.at[slot, c], near[(p + hop) % 3])

    def ici_arrival(p, k, n):
        hop = n.bit_length() - 1
        c = PART_BASE[p] + k
        return remote(place(p, k, n), place(p, k, n), is_.at[n, c], ir.at[n, c], near[(p + hop) % 3])

    def die(p, k, n):
        c = PART_BASE[p] + k
        return remote(source(p, k, n), place(p, k, n), ds_.at[n, c], dr.at[n, c], partner)

    def die_arrival(p, k, n):
        c = PART_BASE[p] + k
        there = place(p, k, n, partner)
        return remote(there, there, ds_.at[n, c], dr.at[n, c], partner)

    def each(fn):
        def one(k, _):
            for p in range(3):
                fn(p, k)
            return 0
        lax.fori_loop(0, 4, one, 0)
        fn(2, 4)

    for hop in range(3):
        each(lambda p, k: ici(p, k, hop, 0).start())
    each(lambda p, k: die(p, k, 0).start())
    own = pltpu.make_async_copy(mine.at[pl.ds(0, UNITS)], out.at[pl.ds(me * UNITS, UNITS)], lsem)
    own.start()

    def forward(n, hops):
        def fn(p, k):
            ici_arrival(p, k, n).wait_recv()
            for hop in hops:
                ici(p, k, hop, n).start()
            die(p, k, n).start()
        return fn

    each(forward(1, (1, 2)))
    each(forward(2, (2,)))
    each(forward(4, ()))
    each(forward(3, (2,)))
    each(forward(5, ()))
    each(forward(6, ()))
    each(forward(7, ()))
    for n in range(8):
        each(lambda p, k: die_arrival(p, k, n).wait_recv())
        each(lambda p, k: die(p, k, n).wait_send())
    for hop in range(3):
        for n in range(1 << hop):
            each(lambda p, k: ici(p, k, hop, n).wait_send())
    own.wait()


def all_gather(mine):
    dma = pltpu.SemaphoreType.DMA
    return pl.pallas_call(
        ag_kernel,
        out_shape=jax.ShapeDtypeStruct((NDEV * UNITS, 4, LANES), jnp.bfloat16),
        in_specs=[pl.BlockSpec(memory_space=pltpu.VMEM)],
        out_specs=pl.BlockSpec(memory_space=pl.ANY),
        scratch_shapes=[dma((8, AG_CHUNKS)), dma((8, AG_CHUNKS)), dma((8, AG_CHUNKS)), dma((8, AG_CHUNKS)), dma(())],
        compiler_params=pltpu.CompilerParams(collective_id=1, has_side_effects=True),
        name='all_gather',
    )(mine)


def solution(mesh):
    def local_step(grad_row, master, mom_first, mom_second, decay_mask, learn_rate):
        g, parts, _ = reduce_scatter(grad_row)
        p, w, m, v, norm = adam(learn_rate, parts, g, master, mom_first, mom_second, decay_mask)
        params = all_gather(p.reshape(ROWS_PAD // 4, 4, LANES))
        return params.reshape(-1), w.reshape(-1), m.reshape(-1), v.reshape(-1), norm[0, 0:1]

    return jax.shard_map(local_step, mesh=mesh, in_specs=(P('dp', None), P('dp'), P('dp'), P('dp'), P('dp'), P()), out_specs=(P(), P('dp'), P('dp'), P('dp'), P()), check_vma=False)
```

```python
import jax
import jax.numpy as jnp
from jax import lax
from jax.experimental import pallas as pl
from jax.experimental.pallas import tpu as pltpu
from jax.sharding import PartitionSpec as P

BETA_FIRST = 0.9
BETA_SECOND = 0.95
ADAM_EPS = 1e-8
CLIP_EPS = 1e-6
WEIGHT_DECAY = 0.1
ADAM_STEP = 10

NDEV = 16
LANES = 128
ROWS = 6908
ROWS_PAD = 6912
CHUNKS = 12
CR = 576
CW = CR * LANES
SLAB = 72
NSLAB = CR // SLAB
DEPTH = 4
UNITS = ROWS // 4
AG_UNITS = 144

MESH = pl.DeviceIdType.MESH


def weight(axis):
    return 2 + axis + axis * axis


def step_of(me, axis):
    w = weight(axis)
    return (1 - 2 * ((me // w) % 2)) * w


def chunk_row(q):
    return CR * q - 4 * (q // (CHUNKS - 1))


def remote(src, dst, ssem, rsem, dev):
    return pltpu.make_async_remote_copy(src_ref=src, dst_ref=dst, send_sem=ssem, recv_sem=rsem, device_id=(dev,), device_id_type=MESH)


def rs_kernel(grad, gout, parts_out, prow, own, par, sb, r1, r2, r3, acc, nrm, psend, precv, s1s, s1r, s2s, s2r, s3s, s3r, ns, nr, lo, lp):
    me = lax.axis_index('dp')
    core = me % 2
    partner = me + 1 - 2 * core

    barrier = pltpu.get_barrier_semaphore()

    def greet(i, _):
        other = lax.rem(me + i, NDEV)
        pl.semaphore_signal(barrier, inc=1, device_id=(other,), device_id_type=MESH)
        return 0

    lax.fori_loop(1, NDEV, greet, 0)
    pl.semaphore_wait(barrier, NDEV - 1)

    def decode(phase, t):
        p = t % 3
        j = t // 3
        if phase == 1:
            o1, o2, o3, k = 1, j % 2, (j // 2) % 2, j // 4
        elif phase == 2:
            o1, o2, o3, k = 0, 1, j % 2, j // 2
        elif phase == 3:
            o1, o2, o3, k = 0, 0, 1, j
        else:
            o1, o2, o3, k = 0, 0, 0, j
        a1, a2, a3 = p, (p + 1) % 3, (p + 2) % 3
        shift = o1 * step_of(me, a1) + o2 * step_of(me, a2) + o3 * step_of(me, a3)
        return p, j, k, a1, a2, a3, shift, 4 * p + k

    base_of = {1: 0, 2: 48, 3: 72, 4: 84}
    count_of = {1: 48, 2: 24, 3: 12, 4: 12}

    def grad_slice(block, q):
        start = pl.multiple_of((block * ROWS + chunk_row(q)) * LANES, LANES)
        return grad.at[:, pl.ds(start, CW)]

    def partner_copy(phase, t):
        _, _, _, _, _, _, shift, q = decode(phase, t)
        s = base_of[phase] + t
        return remote(grad_slice(partner + shift, q), prow.at[s], psend.at[s], precv.at[s], partner)

    for phase in (1, 2, 3, 4):
        def send_rows(t, _, phase=phase):
            partner_copy(phase, t).start()
            return 0
        lax.fori_loop(0, count_of[phase], send_rows, 0)

    def loads(phase, t):
        _, _, _, _, _, _, shift, q = decode(phase, t)
        slot = t % DEPTH
        return (pltpu.make_async_copy(grad_slice(me + shift, q), own.at[slot], lo.at[slot]),
                pltpu.make_async_copy(prow.at[base_of[phase] + t], par.at[slot], lp.at[slot]))

    def start_loads(phase, t):
        partner_copy(phase, t).wait_recv()
        a, b = loads(phase, t)
        a.start()
        b.start()

    def chip_sum(slot, i):
        lo_col = i * SLAB * LANES
        if not isinstance(lo_col, int):
            lo_col = pl.multiple_of(lo_col, SLAB * LANES)
        cols = pl.ds(lo_col, SLAB * LANES)
        v = own[slot, :, cols].astype(jnp.float32) + par[slot, :, cols].astype(jnp.float32)
        return v.reshape(SLAB, LANES)

    def s1_copy(t):
        p, j, k, a1, a2, a3, _, q = decode(1, t)
        return remote(sb.at[t], r1.at[t], s1s.at[t], s1r.at[t], me + step_of(me, a1))

    def r1_at(p, k, o2, o3):
        return ((k * 4) + o3 * 2 + o2) * 3 + p

    def r2_at(p, k, o3):
        return (k * 2 + o3) * 3 + p

    def s2_copy(t):
        p, j, k, a1, a2, a3, _, q = decode(2, t)
        return remote(r1.at[r1_at(p, k, 1, j % 2)], r2.at[t], s2s.at[t], s2r.at[t], me + step_of(me, a2))

    def s3_copy(t):
        p, j, k, a1, a2, a3, _, q = decode(3, t)
        return remote(r2.at[r2_at(p, k, 1)], r3.at[t], s3s.at[t], s3r.at[t], me + step_of(me, a3))

    def run_phase(phase, body, last=None):
        n = count_of[phase]
        for t in range(DEPTH - 1):
            start_loads(phase, t)

        def one(t, _):
            @pl.when(t + DEPTH - 1 < n)
            def _():
                start_loads(phase, t + DEPTH - 1)
            a, b = loads(phase, t)
            a.wait()
            b.wait()
            body(t)
            return 0

        lax.fori_loop(0, n if last is None else n - 1, one, 0)
        if last is not None:
            a, b = loads(phase, n - 1)
            a.wait()
            b.wait()
            last(n - 1)

    def slabs(fn):
        def one(i, _):
            fn(i, pl.ds(pl.multiple_of(i * SLAB, SLAB), SLAB))
            return 0
        lax.fori_loop(0, NSLAB, one, 0)

    def phase1(t):
        slot = t % DEPTH

        def fn(i, rows):
            sb[t, rows, :] = chip_sum(slot, i)
        slabs(fn)
        s1_copy(t).start()

    def phase2(t):
        slot = t % DEPTH
        p, j, k, *_ = decode(2, t)
        src = r1_at(p, k, 1, j % 2)
        s1_copy(src).wait_recv()

        def fn(i, rows):
            r1[src, rows, :] = chip_sum(slot, i) + r1[src, rows, :]
        slabs(fn)
        s2_copy(t).start()

    def phase3(t):
        slot = t % DEPTH
        p, j, k, *_ = decode(3, t)
        s1 = r1_at(p, k, 0, 1)
        s2 = r2_at(p, k, 1)
        s1_copy(s1).wait_recv()
        s2_copy(s2).wait_recv()

        def fn(i, rows):
            r2[s2, rows, :] = chip_sum(slot, i) + r1[s1, rows, :] + r2[s2, rows, :]
        slabs(fn)
        s3_copy(t).start()

    acc[...] = jnp.zeros_like(acc)

    def final_sum(t):
        slot = t % DEPTH
        p, j, k, *_ = decode(4, t)
        s1 = r1_at(p, k, 0, 0)
        s2 = r2_at(p, k, 0)
        s1_copy(s1).wait_recv()
        s2_copy(s2).wait_recv()
        s3_copy(t).wait_recv()

        def value(i, rows):
            v = chip_sum(slot, i) + r1[s1, rows, :] + r2[s2, rows, :] + r3[t, rows, :]
            return v * (1.0 / NDEV)
        return value, 4 * p + k

    def phase4(t):
        value, q = final_sum(t)

        def fn(i, rows):
            v = value(i, rows)
            gout[pl.ds(pl.multiple_of(q * CR + i * SLAB, 8), SLAB), :] = v
            acc[...] += jnp.sum((v * v).reshape(SLAB // 8, 8, LANES), axis=0)
        slabs(fn)

    def phase4_last(t):
        value, _ = final_sum(t)
        start = chunk_row(CHUNKS - 1)
        for i in range(NSLAB):
            v = value(i, pl.ds(i * SLAB, SLAB))
            gout[start + i * SLAB:start + (i + 1) * SLAB, :] = v
            sq = v * v
            if i == 0:
                row = lax.broadcasted_iota(jnp.int32, (SLAB, LANES), 0)
                sq = jnp.where(row < 4, 0.0, sq)
            acc[...] += jnp.sum(sq.reshape(SLAB // 8, 8, LANES), axis=0)

    run_phase(1, phase1)
    run_phase(2, phase2)
    run_phase(3, phase3)
    run_phase(4, phase4, phase4_last)

    nrm[me] = acc[...]

    def norm_copy(i):
        other = lax.rem(me + i, NDEV)
        return remote(acc, nrm.at[me], ns.at[i], nr.at[me], other)

    def norm_arrival(i):
        other = lax.rem(me + i, NDEV)
        return remote(acc, nrm.at[other], ns.at[i], nr.at[other], other)

    def norm_send(i, _):
        norm_copy(i).start()
        return 0

    def norm_wait(i, _):
        norm_arrival(i).wait_recv()
        return 0

    lax.fori_loop(1, NDEV, norm_send, 0)

    def drain(n, copy):
        def one(t, _):
            copy(t).wait_send()
            return 0
        lax.fori_loop(0, n, one, 0)

    for phase in (1, 2, 3, 4):
        drain(count_of[phase], lambda t, phase=phase: partner_copy(phase, t))
    drain(48, s1_copy)
    drain(24, s2_copy)
    drain(12, s3_copy)
    lax.fori_loop(1, NDEV, norm_wait, 0)
    drain(NDEV - 1, lambda t: norm_copy(t + 1))
    total = nrm[0]
    for d in range(1, NDEV):
        total = total + nrm[d]
    parts_out[...] = total


def reduce_scatter(grad):
    f32 = jnp.float32
    dma = pltpu.SemaphoreType.DMA
    return pl.pallas_call(
        rs_kernel,
        out_shape=(pltpu.VMEM((ROWS_PAD, LANES), f32), pltpu.VMEM((8, LANES), f32), jax.ShapeDtypeStruct((96, 1, CW), jnp.bfloat16)),
        in_specs=[pl.BlockSpec(memory_space=pl.ANY)],
        out_specs=(pl.BlockSpec(memory_space=pltpu.VMEM), pl.BlockSpec(memory_space=pltpu.VMEM), pl.BlockSpec(memory_space=pl.ANY)),
        scratch_shapes=[
            pltpu.VMEM((DEPTH, 1, CW), jnp.bfloat16),
            pltpu.VMEM((DEPTH, 1, CW), jnp.bfloat16),
            pltpu.VMEM((48, CR, LANES), f32),
            pltpu.VMEM((48, CR, LANES), f32),
            pltpu.VMEM((24, CR, LANES), f32),
            pltpu.VMEM((12, CR, LANES), f32),
            pltpu.VMEM((8, LANES), f32),
            pltpu.VMEM((NDEV, 8, LANES), f32),
            dma((96,)), dma((96,)),
            dma((48,)), dma((48,)),
            dma((24,)), dma((24,)),
            dma((12,)), dma((12,)),
            dma((NDEV,)), dma((NDEV,)),
            dma((DEPTH,)), dma((DEPTH,)),
        ],
        compiler_params=pltpu.CompilerParams(collective_id=0, has_side_effects=True, vmem_limit_bytes=56 * 1024 * 1024),
        name='reduce_scatter',
    )(grad)


def adam_slab(lr, clip, g, w, m, v, mask):
    h = g * clip
    m_new = BETA_FIRST * m + (1.0 - BETA_FIRST) * h
    v_new = BETA_SECOND * v + (1.0 - BETA_SECOND) * h * h
    step_dir = (m_new / (1.0 - BETA_FIRST ** ADAM_STEP)) / (jnp.sqrt(v_new / (1.0 - BETA_SECOND ** ADAM_STEP)) + ADAM_EPS)
    w_new = w - lr * (step_dir + WEIGHT_DECAY * mask.astype(jnp.float32) * w)
    return w_new, m_new, v_new


def ag_kernel(lr, parts, g, w_in, m_in, v_in, mask_in, w, m, v, norm_out, out, mask, is_, ir, ds_, dr, ld):
    me = lax.axis_index('dp')
    partner = me + 1 - 2 * (me % 2)
    barrier = pltpu.get_barrier_semaphore()
    near = [me + step_of(me, a) for a in range(3)]
    for other in near + [partner]:
        pl.semaphore_signal(barrier, inc=1, device_id=(other,), device_id_type=MESH)

    def loads(q, size=CR):
        start = q * CR
        if not isinstance(start, int):
            start = pl.multiple_of(start, 8)
        rows = pl.ds(start, size)
        pairs = ((w_in, w), (m_in, m), (v_in, v), (mask_in, mask))
        return [pltpu.make_async_copy(a.at[rows], b.at[rows], ld.at[i, q]) for i, (a, b) in enumerate(pairs)]

    def each(fn, first=0):
        def one(k, _):
            for p in range(3):
                fn(p, k, AG_UNITS)
            return 0
        lax.fori_loop(first, 3, one, 0)
        fn(0, 3, AG_UNITS)
        fn(1, 3, AG_UNITS)
        fn(2, 3, UNITS - 11 * AG_UNITS)

    def start_loads(p, k, units):
        for c in loads(4 * p + k, 4 * units):
            c.start()

    each(start_loads)

    norm = jnp.sqrt(jnp.sum(parts[...], keepdims=True))
    norm_out[...] = jnp.broadcast_to(norm, norm_out.shape)
    clip = jnp.minimum(1.0, 1.0 / (norm + CLIP_EPS))

    def place(p, k, units, n, dev=me):
        a = [p, (p + 1) % 3, (p + 2) % 3]
        block = dev
        for bit in range(3):
            if (n >> bit) & 1:
                block = block + step_of(me, a[bit])
        return out.at[pl.ds(block * UNITS + AG_UNITS * (4 * p + k), units)]

    def ici(p, k, units, hop, n):
        slot = n | (1 << hop)
        c = 4 * p + k
        here = place(p, k, units, n)
        return remote(here, here, is_.at[slot, c], ir.at[slot, c], near[(p + hop) % 3])

    def ici_arrival(p, k, units, n):
        hop = n.bit_length() - 1
        c = 4 * p + k
        here = place(p, k, units, n)
        return remote(here, here, is_.at[n, c], ir.at[n, c], near[(p + hop) % 3])

    def die(p, k, units, n):
        c = 4 * p + k
        here = place(p, k, units, n)
        return remote(here, here, ds_.at[n, c], dr.at[n, c], partner)

    def die_arrival(p, k, units, n):
        c = 4 * p + k
        there = place(p, k, units, n, partner)
        return remote(there, there, ds_.at[n, c], dr.at[n, c], partner)

    def update(p, k, units):
        q = 4 * p + k
        for c in loads(q, 4 * units):
            c.wait()
        rate = lr[0]

        def slab(row0, n):
            rows = pl.ds(row0, n)
            w_new, m_new, v_new = adam_slab(rate, clip, g[rows, :], w[rows, :], m[rows, :], v[rows, :], mask[rows, :])
            w[rows, :] = w_new
            m[rows, :] = m_new
            v[rows, :] = v_new
            return w_new.astype(jnp.bfloat16).reshape(n // 4, 4, LANES)

        whole = (4 * units) // SLAB

        def one(i, _):
            out[pl.ds(me * UNITS + q * AG_UNITS + i * (SLAB // 4), SLAB // 4)] = slab(pl.multiple_of(q * CR + i * SLAB, 8), SLAB)
            return 0
        lax.fori_loop(0, whole, one, 0)
        rest = 4 * units - whole * SLAB
        if rest:
            out[pl.ds(me * UNITS + q * AG_UNITS + whole * (SLAB // 4), rest // 4)] = slab(q * CR + whole * SLAB, rest)

    for p in range(3):
        update(p, 0, AG_UNITS)
        if p == 0:
            pl.semaphore_wait(barrier, 4)
        for hop in range(3):
            ici(p, 0, AG_UNITS, hop, 0).start()
        die(p, 0, AG_UNITS, 0).start()

    def later(p, k, units):
        update(p, k, units)
        ici(p, k, units, 0, 0).start()

    each(later, 1)
    for hop in (1, 2):
        each(lambda p, k, units: ici(p, k, units, hop, 0).start(), 1)
    each(lambda p, k, units: die(p, k, units, 0).start(), 1)

    def forward(n, hops):
        def fn(p, k, units):
            ici_arrival(p, k, units, n).wait_recv()
            for hop in hops:
                ici(p, k, units, hop, n).start()
            die(p, k, units, n).start()
        return fn

    each(forward(1, (1, 2)))
    each(forward(2, (2,)))
    each(forward(4, ()))
    each(forward(3, (2,)))
    each(forward(5, ()))
    each(forward(6, ()))
    each(forward(7, ()))
    for n in range(8):
        each(lambda p, k, units: die_arrival(p, k, units, n).wait_recv())
        each(lambda p, k, units: die(p, k, units, n).wait_send())
    for hop in range(3):
        for n in range(1 << hop):
            each(lambda p, k, units: ici(p, k, units, hop, n).wait_send())


def adam_gather(lr, parts, g, w, m, v, mask):
    f32 = jnp.float32
    dma = pltpu.SemaphoreType.DMA
    flat = lambda a: pltpu.with_memory_space_constraint(a.reshape(ROWS, LANES), pltpu.HBM)
    hbm = pl.BlockSpec(memory_space=pl.ANY)
    vmem = pl.BlockSpec(memory_space=pltpu.VMEM)
    state = pltpu.VMEM((ROWS, LANES), f32)
    return pl.pallas_call(
        ag_kernel,
        out_shape=(state, state, state, jax.ShapeDtypeStruct((8, LANES), f32), pltpu.VMEM((NDEV * UNITS, 4, LANES), jnp.bfloat16)),
        in_specs=[pl.BlockSpec(memory_space=pltpu.SMEM), vmem, vmem, hbm, hbm, hbm, hbm],
        out_specs=(vmem, vmem, vmem, vmem, vmem),
        scratch_shapes=[pltpu.VMEM((ROWS, LANES), jnp.int32), dma((8, CHUNKS)), dma((8, CHUNKS)), dma((8, CHUNKS)), dma((8, CHUNKS)), dma((4, CHUNKS))],
        compiler_params=pltpu.CompilerParams(collective_id=1, has_side_effects=True, vmem_limit_bytes=8 * 1024 * 1024),
        name='adam_gather',
    )(lr, pltpu.with_memory_space_constraint(parts, pltpu.VMEM), pltpu.with_memory_space_constraint(g, pltpu.VMEM), flat(w), flat(m), flat(v), flat(mask))


PUBLISH_PIECES = 8


def publish_kernel(p_in, w_in, m_in, v_in, n_in, p_out, w_out, m_out, v_out, n_out, big, small):
    size = NDEV * UNITS // PUBLISH_PIECES
    copies = [pltpu.make_async_copy(p_in.at[pl.ds(i * size, size)], p_out.at[pl.ds(i * size, size)], big.at[i]) for i in range(PUBLISH_PIECES)]
    copies += [pltpu.make_async_copy(a, b, small.at[i]) for i, (a, b) in enumerate(((w_in, w_out), (m_in, m_out), (v_in, v_out)))]
    for c in copies:
        c.start()
    n_out[...] = n_in[0, 0:1]
    for c in copies:
        c.wait()


def publish(arrays, norm):
    dma = pltpu.SemaphoreType.DMA
    vmem = pl.BlockSpec(memory_space=pltpu.VMEM)
    hbm = pl.BlockSpec(memory_space=pl.ANY)
    arrays = [pltpu.with_memory_space_constraint(a, pltpu.VMEM) for a in arrays]
    return pl.pallas_call(
        publish_kernel,
        out_shape=[jax.ShapeDtypeStruct(a.shape, a.dtype) for a in arrays] + [jax.ShapeDtypeStruct((1,), jnp.float32)],
        in_specs=[vmem] * 5,
        out_specs=[hbm] * 4 + [vmem],
        scratch_shapes=[dma((PUBLISH_PIECES,)), dma((3,))],
        compiler_params=pltpu.CompilerParams(vmem_limit_bytes=1024 * 1024),
        name='publish',
    )(*arrays, norm)


def solution(mesh):
    def local_step(grad_row, master, mom_first, mom_second, decay_mask, learn_rate):
        g, parts, _ = reduce_scatter(grad_row)
        w, m, v, norm, params = adam_gather(learn_rate, parts, g, master, mom_first, mom_second, decay_mask)
        params, w, m, v, norm = publish([params, w, m, v], norm)
        return params.reshape(-1), w.reshape(-1), m.reshape(-1), v.reshape(-1), norm

    return jax.shard_map(local_step, mesh=mesh, in_specs=(P('dp', None), P('dp'), P('dp'), P('dp'), P('dp'), P()), out_specs=(P(), P('dp'), P('dp'), P('dp'), P()), check_vma=False)
```

```python
import jax
import jax.numpy as jnp
from jax import lax
from jax.experimental import pallas as pl
from jax.experimental.pallas import tpu as pltpu
from jax.sharding import PartitionSpec as P

BETA_FIRST = 0.9
BETA_SECOND = 0.95
ADAM_EPS = 1e-8
CLIP_EPS = 1e-6
WEIGHT_DECAY = 0.1
ADAM_STEP = 10

NDEV = 16
LANES = 128
ROWS = 6908
ROWS_PAD = 6912
CHUNKS = 12
CR = 576
CW = CR * LANES
SLAB = 72
NSLAB = CR // SLAB
DEPTH = 4
SENDS = 24
UNITS = ROWS // 4
LATE = 12
AG_UNITS = 144

MESH = pl.DeviceIdType.MESH


def weight(axis):
    return 2 + axis + axis * axis


def step_of(me, axis):
    w = weight(axis)
    return (1 - 2 * ((me // w) % 2)) * w


def chunk_row(q):
    return CR * q - 4 * (q // (CHUNKS - 1))


def remote(src, dst, ssem, rsem, dev):
    return pltpu.make_async_remote_copy(src_ref=src, dst_ref=dst, send_sem=ssem, recv_sem=rsem, device_id=(dev,), device_id_type=MESH)


def adam_slab(lr, clip, g, w, m, v, mask):
    h = g * clip
    m_new = BETA_FIRST * m + (1.0 - BETA_FIRST) * h
    v_new = BETA_SECOND * v + (1.0 - BETA_SECOND) * h * h
    step_dir = (m_new / (1.0 - BETA_FIRST ** ADAM_STEP)) / (jnp.sqrt(v_new / (1.0 - BETA_SECOND ** ADAM_STEP)) + ADAM_EPS)
    w_new = w - lr * (step_dir + WEIGHT_DECAY * mask.astype(jnp.float32) * w)
    return w_new, m_new, v_new


def step_kernel(lr, grad, w_in, m_in, v_in, mask_in, w, m, v, norm_out, out, prow, r1, r2,
                own, par, st1, st2, early, mask, sb, r3, acc, nrm,
                psend, precv, sent, s1r, s2r, s3r, ns, nr, lo, lp, l1, l2, ld, is_, ir, ds_, dr):
    me = lax.axis_index('dp')
    partner = me + 1 - 2 * (me % 2)
    near = [me + step_of(me, a) for a in range(3)]

    def decode(phase, t):
        p = t % 3
        j = t // 3
        if phase == 1:
            o1, o2, o3, k = 1, j % 2, (j // 2) % 2, j // 4
        elif phase == 2:
            o1, o2, o3, k = 0, 1, j % 2, j // 2
        elif phase == 3:
            o1, o2, o3, k = 0, 0, 1, j
        else:
            o1, o2, o3, k = 0, 0, 0, j
        a1, a2, a3 = p, (p + 1) % 3, (p + 2) % 3
        shift = o1 * step_of(me, a1) + o2 * step_of(me, a2) + o3 * step_of(me, a3)
        return p, j, k, a1, a2, a3, shift, 4 * p + k

    base_of = {1: 0, 2: 48, 3: 72, 4: 84}
    count_of = {1: 48, 2: 24, 3: 12, 4: 12}

    def grad_slice(block, q):
        start = pl.multiple_of((block * ROWS + chunk_row(q)) * LANES, LANES)
        return grad.at[:, pl.ds(start, CW)]

    def early_copy(t):
        _, _, _, _, _, _, shift, q = decode(1, t)
        return remote(grad_slice(partner + shift, q), early.at[t], psend, precv.at[LATE + 1 + t], partner)

    def partner_copy(phase, t):
        _, _, _, _, _, _, shift, q = decode(phase, t)
        group = t // DEPTH if phase == 1 else LATE
        return remote(grad_slice(partner + shift, q), prow.at[base_of[phase] + t], psend, precv.at[group], partner)

    def rows_here(first, count, group):
        rows = prow.at[pl.ds(first, count)]
        return remote(rows, rows, psend, precv.at[group], partner)

    def own_load(phase, t):
        _, _, _, _, _, _, shift, q = decode(phase, t)
        slot = t % DEPTH
        return pltpu.make_async_copy(grad_slice(me + shift, q), own.at[slot], lo.at[slot])

    def s1_copy(t):
        p, j, k, *_ = decode(1, t)
        return remote(sb.at[t % SENDS], r1.at[(4 * p + k) * 4 + j % 4], sent.at[t % SENDS], s1r.at[4 * p + k], me + step_of(me, p))

    def s2_copy(t):
        p, j, k, *_ = decode(2, t)
        return remote(sb.at[t % SENDS], r2.at[(4 * p + k) * 2 + j % 2], sent.at[t % SENDS], s2r.at[4 * p + k], me + step_of(me, (p + 1) % 3))

    def s3_copy(t):
        p, j, k, *_ = decode(3, t)
        return remote(sb.at[t % SENDS], r3.at[t], sent.at[t % SENDS], s3r.at[t], me + step_of(me, (p + 2) % 3))

    def s1_group(q):
        rows = r1.at[pl.ds(q * 4, 4)]
        return remote(rows, rows, sent.at[0], s1r.at[q], partner)

    def s2_group(q):
        rows = r2.at[pl.ds(q * 2, 2)]
        return remote(rows, rows, sent.at[0], s2r.at[q], partner)

    def r1_at(p, k, o2, o3):
        return (4 * p + k) * 4 + o3 * 2 + o2

    def r2_at(p, k, o3):
        return (4 * p + k) * 2 + o3

    def sources(phase, t):
        p, j, k, *_ = decode(phase, t)
        if phase == 2:
            return r1_at(p, k, 1, j % 2), None
        if phase == 3:
            return r1_at(p, k, 0, 1), r2_at(p, k, 1)
        return r1_at(p, k, 0, 0), r2_at(p, k, 0)

    def loads(phase, t):
        slot = t % DEPTH
        copies = [own_load(phase, t), pltpu.make_async_copy(prow.at[base_of[phase] + t], par.at[slot], lp.at[slot])]
        if phase > 1:
            i1, i2 = sources(phase, t)
            copies.append(pltpu.make_async_copy(r1.at[i1], st1.at[slot], l1.at[slot]))
            if phase > 2:
                copies.append(pltpu.make_async_copy(r2.at[i2], st2.at[slot], l2.at[slot]))
        return copies

    def start_loads(phase, t):
        p, j, k, *_ = decode(phase, t)
        if phase == 1:
            if isinstance(t, int):
                if t % DEPTH == 0:
                    rows_here(t, DEPTH, t // DEPTH).wait_recv()
            else:
                @pl.when(t % DEPTH == 0)
                def _():
                    rows_here(t, DEPTH, t // DEPTH).wait_recv()
        elif phase == 2:
            if isinstance(j, int):
                if j % 2 == 0:
                    s1_group(4 * p + k).wait_recv()
            else:
                @pl.when(j % 2 == 0)
                def _():
                    s1_group(4 * p + k).wait_recv()
        elif phase == 3:
            s2_group(4 * p + k).wait_recv()
        for c in loads(phase, t):
            c.start()

    def chip_sum(slot, i, rows_of=None):
        rows_of = par if rows_of is None else rows_of
        cols = pl.ds(pl.multiple_of(i * (SLAB * LANES), SLAB * LANES), SLAB * LANES)
        total = own[slot, :, cols].astype(jnp.float32) + rows_of[slot, :, cols].astype(jnp.float32)
        return total.reshape(SLAB, LANES)

    def slabs(fn):
        def one(i, _):
            fn(i, pl.ds(pl.multiple_of(i * SLAB, SLAB), SLAB))
            return 0
        lax.fori_loop(0, NSLAB, one, 0)

    def loop(lo_t, hi_t, fn):
        def one(t, _):
            fn(t)
            return 0
        lax.fori_loop(lo_t, hi_t, one, 0)

    def run_phase(phase, body, first=0):
        n = count_of[phase]
        for t in range(DEPTH - 1):
            start_loads(phase, first + t)

        def one(t):
            @pl.when(t + DEPTH - 1 < n)
            def _():
                start_loads(phase, t + DEPTH - 1)
            for c in loads(phase, t):
                c.wait()
            body(t)
        loop(first, n, one)

    barrier = pltpu.get_barrier_semaphore()
    for other in [partner] + near:
        pl.semaphore_signal(barrier, inc=1, device_id=(other,), device_id_type=MESH)
    for t in range(DEPTH):
        own_load(1, t).start()
    pl.semaphore_wait(barrier, 4)

    for t in range(DEPTH):
        early_copy(t).start()
    loop(DEPTH, 16, lambda t: partner_copy(1, t).start())
    for t in range(DEPTH):
        own_load(1, t).wait()
        early_copy(t).wait_recv()

        def fn(i, rows):
            sb[t, rows, :] = chip_sum(t, i, early)
        slabs(fn)
        s1_copy(t).start()
    loop(16, 48, lambda t: partner_copy(1, t).start())

    def phase1(t):
        @pl.when(t >= SENDS)
        def _():
            s1_copy(t - SENDS).wait_send()
        slot = t % DEPTH

        def fn(i, rows):
            sb[t % SENDS, rows, :] = chip_sum(slot, i)
        slabs(fn)
        s1_copy(t).start()

    def phase2(t):
        s1_copy(t + SENDS).wait_send()
        slot = t % DEPTH

        def fn(i, rows):
            sb[t % SENDS, rows, :] = chip_sum(slot, i) + st1[slot, rows, :]
        slabs(fn)
        s2_copy(t).start()

    def phase3(t):
        s2_copy(t).wait_send()
        slot = t % DEPTH

        def fn(i, rows):
            sb[t % SENDS, rows, :] = chip_sum(slot, i) + st1[slot, rows, :] + st2[slot, rows, :]
        slabs(fn)
        s3_copy(t).start()

    acc[...] = jnp.zeros_like(acc)

    def phase4(t):
        slot = t % DEPTH
        p, j, k, *_ = decode(4, t)
        skip = 4 * ((4 * p + k) // (CHUNKS - 1))
        s3_copy(t).wait_recv()

        def fn(i, rows):
            g = (chip_sum(slot, i) + st1[slot, rows, :] + st2[slot, rows, :] + r3[t, rows, :]) * (1.0 / NDEV)
            r3[t, rows, :] = g
            row = lax.broadcasted_iota(jnp.int32, (SLAB, LANES), 0) + i * SLAB
            acc[...] += jnp.sum(jnp.where(row < skip, 0.0, g * g).reshape(SLAB // 8, 8, LANES), axis=0)
        slabs(fn)

    run_phase(1, phase1, DEPTH)
    for phase in (2, 3, 4):
        loop(0, count_of[phase], lambda t, phase=phase: partner_copy(phase, t).start())
    rows_here(48, 48, LATE).wait_recv()

    states = [pltpu.make_async_copy(a, b, ld.at[i]) for i, (a, b) in enumerate(((w_in, w), (m_in, m), (v_in, v), (mask_in, mask)))]
    for c in states:
        c.start()
    run_phase(2, phase2)
    for c in states:
        c.wait()
    rows_here(DEPTH, 96 - DEPTH, LATE).wait_send()
    remote(early, early, psend, precv.at[0], partner).wait_send()
    run_phase(3, phase3)
    loop(12, 24, lambda t: s2_copy(t).wait_send())
    run_phase(4, phase4)

    nrm[me] = acc[...]

    def norm_copy(i):
        return remote(acc, nrm.at[me], ns, nr, lax.rem(me + i, NDEV))

    others = nrm.at[pl.ds(0, NDEV - 1)]
    all_norms = remote(others, others, ns, nr, partner)

    loop(1, NDEV, lambda i: norm_copy(i).start())
    loop(0, 12, lambda t: s3_copy(t).wait_send())
    all_norms.wait_recv()
    total = nrm[0]
    for i in range(1, NDEV):
        total = total + nrm[i]
    norm = jnp.sqrt(jnp.sum(total, keepdims=True))
    norm_out[...] = jnp.broadcast_to(norm, norm_out.shape)
    clip = jnp.minimum(1.0, 1.0 / (norm + CLIP_EPS))
    rate = lr[0]

    def each(fn, first=0):
        def one(k, _):
            for p in range(3):
                fn(p, k, AG_UNITS)
            return 0
        lax.fori_loop(first, 3, one, 0)
        fn(0, 3, AG_UNITS)
        fn(1, 3, AG_UNITS)
        fn(2, 3, UNITS - 11 * AG_UNITS)

    def block_of(p, n):
        a = [p, (p + 1) % 3, (p + 2) % 3]
        block = me
        for bit in range(3):
            if (n >> bit) & 1:
                block = block + step_of(me, a[bit])
        return block

    def place(p, k, units, n):
        return out.at[pl.ds(block_of(p, n) * UNITS + AG_UNITS * (4 * p + k), units)]

    def place_part(p, n):
        units = 4 * AG_UNITS if p < 2 else UNITS - 8 * AG_UNITS
        return out.at[pl.ds(block_of(p, n) * UNITS + 4 * AG_UNITS * p, units)]

    def ir_index(p, k, n):
        if n in (4, 5, 6):
            return 48 + 3 * (n - 4) + p
        return 12 * (n if n < 4 else 0) + 4 * p + k

    def ici(p, k, units, hop, n):
        here = place(p, k, units, n)
        return remote(here, here, is_, ir.at[ir_index(p, k, n | (1 << hop))], near[(p + hop) % 3])

    def ici_arrival(p, k, units, n):
        here = place(p, k, units, n)
        return remote(here, here, is_, ir.at[ir_index(p, k, n)], partner)

    def part_arrival(p, n):
        here = place_part(p, n)
        return remote(here, here, is_, ir.at[ir_index(p, 0, n)], partner)

    def die(here):
        return remote(here, here, ds_, dr, partner)

    def update(p, k, units):
        q = 4 * p + k
        t = 3 * k + p
        short = units != AG_UNITS

        def slab(row0, n):
            rows = pl.ds(row0 + q * CR, n)
            src = pl.ds(row0 + 4, n) if short else pl.ds(row0, n)
            w_new, m_new, v_new = adam_slab(rate, clip, r3[t, src, :], w[rows, :], m[rows, :], v[rows, :], mask[rows, :])
            w[rows, :] = w_new
            m[rows, :] = m_new
            v[rows, :] = v_new
            return w_new.astype(jnp.bfloat16).reshape(n // 4, 4, LANES)

        base = me * UNITS + q * AG_UNITS
        whole = (4 * units) // SLAB
        if short:
            for i in range(whole):
                out[pl.ds(base + i * (SLAB // 4), SLAB // 4)] = slab(i * SLAB, SLAB)
            rest = 4 * units - whole * SLAB
            out[pl.ds(base + whole * (SLAB // 4), rest // 4)] = slab(whole * SLAB, rest)
        else:
            def one(i, _):
                out[pl.ds(base + i * (SLAB // 4), SLAB // 4)] = slab(pl.multiple_of(i * SLAB, SLAB), SLAB)
                return 0
            lax.fori_loop(0, whole, one, 0)

    for p in range(3):
        update(p, 0, AG_UNITS)
        for hop in range(3):
            ici(p, 0, AG_UNITS, hop, 0).start()

    def later(p, k, units):
        update(p, k, units)
        ici(p, k, units, 0, 0).start()

    each(later, 1)
    for hop in (1, 2):
        each(lambda p, k, units: ici(p, k, units, hop, 0).start(), 1)
    die(out.at[pl.ds(me * UNITS, UNITS)]).start()
    all_norms.wait_send()

    def forward(n, hops):
        def fn(p, k, units):
            ici_arrival(p, k, units, n).wait_recv()
            for hop in hops:
                ici(p, k, units, hop, n).start()
            die(place(p, k, units, n)).start()
        return fn

    def forward_part(n):
        for p in range(3):
            part_arrival(p, n).wait_recv()
            die(place_part(p, n)).start()

    each(forward(1, (1, 2)))
    each(forward(2, (2,)))
    each(forward(3, (2,)))
    forward_part(4)
    forward_part(5)
    forward_part(6)
    each(forward(7, ()))
    sends = out.at[pl.ds(0, 7 * UNITS)]
    remote(sends, sends, is_, ir.at[0], partner).wait_send()
    half = out.at[pl.ds(0, 8 * UNITS)]
    die(half).wait_send()
    die(half).wait_recv()


def step(lr, grad, w, m, v, mask):
    f32, bf16 = jnp.float32, jnp.bfloat16
    dma = pltpu.SemaphoreType.DMA
    flat = lambda a: pltpu.with_memory_space_constraint(a.reshape(ROWS, LANES), pltpu.HBM)
    hbm = pl.BlockSpec(memory_space=pl.ANY)
    vmem = pl.BlockSpec(memory_space=pltpu.VMEM)
    state = pltpu.VMEM((ROWS, LANES), f32)
    return pl.pallas_call(
        step_kernel,
        out_shape=(
            state, state, state, pltpu.VMEM((8, LANES), f32),
            pltpu.VMEM((NDEV * UNITS, 4, LANES), bf16),
            pltpu.HBM((96, 1, CW), bf16), pltpu.HBM((48, CR, LANES), f32), pltpu.HBM((24, CR, LANES), f32),
        ),
        in_specs=[pl.BlockSpec(memory_space=pltpu.SMEM)] + [hbm] * 5,
        out_specs=(vmem, vmem, vmem, vmem, vmem, hbm, hbm, hbm),
        scratch_shapes=[
            pltpu.VMEM((DEPTH, 1, CW), bf16),
            pltpu.VMEM((DEPTH, 1, CW), bf16),
            pltpu.VMEM((DEPTH, CR, LANES), f32),
            pltpu.VMEM((DEPTH, CR, LANES), f32),
            pltpu.VMEM((DEPTH, 1, CW), bf16),
            pltpu.VMEM((ROWS, LANES), jnp.int32),
            pltpu.VMEM((SENDS, CR, LANES), f32),
            pltpu.VMEM((12, CR, LANES), f32),
            pltpu.VMEM((8, LANES), f32),
            pltpu.VMEM((NDEV, 8, LANES), f32),
            dma(()), dma((LATE + 1 + DEPTH,)), dma((SENDS,)),
            dma((12,)), dma((12,)), dma((12,)),
            dma(()), dma(()),
            dma((DEPTH,)), dma((DEPTH,)), dma((DEPTH,)), dma((DEPTH,)),
            dma((4,)),
            dma(()), dma((57,)), dma(()), dma(()),
        ],
        compiler_params=pltpu.CompilerParams(collective_id=0, has_side_effects=True, vmem_limit_bytes=22 * 1024 * 1024),
        name='step',
    )(lr, grad, flat(w), flat(m), flat(v), flat(mask))


PUBLISH_PIECES = 8


def publish_kernel(p_in, w_in, m_in, v_in, n_in, p_out, w_out, m_out, v_out, n_out, big, small):
    size = NDEV * UNITS // PUBLISH_PIECES
    copies = [pltpu.make_async_copy(p_in.at[pl.ds(i * size, size)], p_out.at[pl.ds(i * size, size)], big.at[i]) for i in range(PUBLISH_PIECES)]
    copies += [pltpu.make_async_copy(a, b, small.at[i]) for i, (a, b) in enumerate(((w_in, w_out), (m_in, m_out), (v_in, v_out)))]
    for c in copies:
        c.start()
    n_out[...] = n_in[0, 0:1]
    for c in copies:
        c.wait()


def publish(arrays, norm):
    dma = pltpu.SemaphoreType.DMA
    vmem = pl.BlockSpec(memory_space=pltpu.VMEM)
    hbm = pl.BlockSpec(memory_space=pl.ANY)
    arrays = [pltpu.with_memory_space_constraint(a, pltpu.VMEM) for a in arrays]
    norm = pltpu.with_memory_space_constraint(norm, pltpu.VMEM)
    return pl.pallas_call(
        publish_kernel,
        out_shape=[jax.ShapeDtypeStruct(a.shape, a.dtype) for a in arrays] + [jax.ShapeDtypeStruct((1,), jnp.float32)],
        in_specs=[vmem] * 5,
        out_specs=[hbm] * 4 + [vmem],
        scratch_shapes=[dma((PUBLISH_PIECES,)), dma((3,))],
        compiler_params=pltpu.CompilerParams(vmem_limit_bytes=1024 * 1024),
        name='publish',
    )(*arrays, norm)


def solution(mesh):
    def local_step(grad_row, master, mom_first, mom_second, decay_mask, learn_rate):
        w, m, v, norm, params, *_ = step(learn_rate, grad_row, master, mom_first, mom_second, decay_mask)
        params, w, m, v, norm = publish([params, w, m, v], norm)
        return params.reshape(-1), w.reshape(-1), m.reshape(-1), v.reshape(-1), norm

    return jax.shard_map(local_step, mesh=mesh, in_specs=(P('dp', None), P('dp'), P('dp'), P('dp'), P('dp'), P()), out_specs=(P(), P('dp'), P('dp'), P('dp'), P()), check_vma=False)
```

```python
import jax
import jax.numpy as jnp
from jax import lax
from jax.experimental import pallas as pl
from jax.experimental.pallas import tpu as pltpu
from jax.sharding import PartitionSpec as P

BETA_FIRST = 0.9
BETA_SECOND = 0.95
ADAM_EPS = 1e-8
CLIP_EPS = 1e-6
WEIGHT_DECAY = 0.1
ADAM_STEP = 10

NDEV = 16
LANES = 128
ROWS = 6908
ROWS_PAD = 6912
CHUNKS = 12
CR = 576
CW = CR * LANES
SLAB = 72
NSLAB = CR // SLAB
DEPTH = 4
GROUPS = 6
UNITS = ROWS // 4
LATE = 12
AG_UNITS = 144

MESH = pl.DeviceIdType.MESH


def weight(axis):
    return 2 + axis + axis * axis


def step_of(me, axis):
    w = weight(axis)
    return (1 - 2 * ((me // w) % 2)) * w


def chunk_row(q):
    return CR * q - 4 * (q // (CHUNKS - 1))


def remote(src, dst, ssem, rsem, dev):
    return pltpu.make_async_remote_copy(src_ref=src, dst_ref=dst, send_sem=ssem, recv_sem=rsem, device_id=(dev,), device_id_type=MESH)


def adam_slab(lr, clip, g, w, m, v, mask):
    h = g * clip
    m_new = BETA_FIRST * m + (1.0 - BETA_FIRST) * h
    v_new = BETA_SECOND * v + (1.0 - BETA_SECOND) * h * h
    step_dir = (m_new / (1.0 - BETA_FIRST ** ADAM_STEP)) / (jnp.sqrt(v_new / (1.0 - BETA_SECOND ** ADAM_STEP)) + ADAM_EPS)
    w_new = w - lr * (step_dir + WEIGHT_DECAY * mask.astype(jnp.float32) * w)
    return w_new, m_new, v_new


def step_kernel(lr_in, grad, w_in, m_in, v_in, mask_in, w, m, v, norm_out, out, prow, r1, r2,
                lr, own, par, st1, st2, early, mask, sb, r3, acc, nrm,
                psend, precv, sent, s1r, s2r, s3r, ns, nr, lo, lp, l1, l2, ld, is_, ir, ds_, dr):
    me = lax.axis_index('dp')
    partner = me + 1 - 2 * (me % 2)
    near = [me + step_of(me, a) for a in range(3)]

    base_of = {1: 0, 2: 48, 3: 72, 4: 84}
    count_of = {1: 48, 2: 24, 3: 12, 4: 12}

    def decode(phase, t):
        if phase == 1:
            if isinstance(t, int) and t < 12:
                return t % 3, 0, t // 3
            return (t // 4) % 3, t // 12, t % 4
        if phase == 2:
            return (t // 2) % 3, t // 6, t % 2
        return t % 3, t // 3, 0

    def where(phase, t):
        p, k, j = decode(phase, t)
        if phase == 1:
            o1, o2, o3 = 1, j % 2, j // 2
        elif phase == 2:
            o1, o2, o3 = 0, 1, j
        else:
            o1, o2, o3 = 0, 0, 1 if phase == 3 else 0
        shift = o1 * step_of(me, p) + o2 * step_of(me, (p + 1) % 3) + o3 * step_of(me, (p + 2) % 3)
        return shift, 4 * p + k

    def grad_slice(block, q):
        start = pl.multiple_of((block * ROWS + chunk_row(q)) * LANES, LANES)
        return grad.at[:, pl.ds(start, CW)]

    def early_copy(t):
        shift, q = where(1, t)
        return remote(grad_slice(partner + shift, q), early.at[t], psend, precv.at[LATE + 1 + t], partner)

    def partner_copy(phase, t):
        shift, q = where(phase, t)
        group = t // 4 if phase == 1 else LATE
        return remote(grad_slice(partner + shift, q), prow.at[base_of[phase] + t], psend, precv.at[group], partner)

    def rows_here(first, count, group):
        rows = prow.at[pl.ds(first, count)]
        return remote(rows, rows, psend, precv.at[group], partner)

    def own_load(phase, t):
        shift, q = where(phase, t)
        slot = t % DEPTH
        return pltpu.make_async_copy(grad_slice(me + shift, q), own.at[slot], lo.at[slot])

    def slots(g, count):
        return sb.at[pl.ds(4 * (g % GROUPS), count)]

    def s1_one(p, j):
        return remote(sb.at[4 * p + j], r1.at[16 * p + j], sent.at[p], s1r.at[4 * p], me + step_of(me, p))

    def s1_copy(p, k):
        g = 3 * k + p
        return remote(slots(g, 4), r1.at[pl.ds((4 * p + k) * 4, 4)], sent.at[g % GROUPS], s1r.at[4 * p + k], me + step_of(me, p))

    def s2_copy(p, k):
        g = 3 * k + p
        return remote(slots(g, 2), r2.at[pl.ds((4 * p + k) * 2, 2)], sent.at[g % GROUPS], s2r.at[4 * p + k], me + step_of(me, (p + 1) % 3))

    def s3_copy(p, k):
        g = 3 * k + p
        return remote(sb.at[4 * (g % GROUPS)], r3.at[g], sent.at[g % GROUPS], s3r.at[g], me + step_of(me, (p + 2) % 3))

    def left(g, count):
        here = slots(g, count)
        remote(here, here, sent.at[g % GROUPS], s1r.at[0], partner).wait_send()

    def sources(phase, t):
        p, k, j = decode(phase, t)
        q = 4 * p + k
        if phase == 2:
            return 4 * q + 2 * j + 1, None
        if phase == 3:
            return 4 * q + 2, 2 * q + 1
        return 4 * q, 2 * q

    def loads(phase, t):
        slot = t % DEPTH
        copies = [own_load(phase, t), pltpu.make_async_copy(prow.at[base_of[phase] + t], par.at[slot], lp.at[slot])]
        if phase > 1:
            i1, i2 = sources(phase, t)
            copies.append(pltpu.make_async_copy(r1.at[i1], st1.at[slot], l1.at[slot]))
            if phase > 2:
                copies.append(pltpu.make_async_copy(r2.at[i2], st2.at[slot], l2.at[slot]))
        return copies

    def when(cond, fn):
        if isinstance(cond, bool):
            if cond:
                fn()
        else:
            pl.when(cond)(fn)

    def start_loads(phase, t):
        p, k, j = decode(phase, t)
        if phase == 1:
            when(t % 4 == 0, lambda: rows_here(t, 4, t // 4).wait_recv())
        elif phase == 2:
            when(j == 0, lambda: s1_copy(p, k).wait_recv())
        elif phase == 3:
            s2_copy(p, k).wait_recv()
        for c in loads(phase, t):
            c.start()

    def chip_sum(slot, i, rows_of=None):
        rows_of = par if rows_of is None else rows_of
        cols = pl.ds(pl.multiple_of(i * (SLAB * LANES), SLAB * LANES), SLAB * LANES)
        total = own[slot, :, cols].astype(jnp.float32) + rows_of[slot, :, cols].astype(jnp.float32)
        return total.reshape(SLAB, LANES)

    def slabs(fn):
        def one(i, _):
            fn(i, pl.ds(pl.multiple_of(i * SLAB, SLAB), SLAB))
            return 0
        lax.fori_loop(0, NSLAB, one, 0)

    def loop(lo_t, hi_t, fn):
        def one(t, _):
            fn(t)
            return 0
        lax.fori_loop(lo_t, hi_t, one, 0)

    def run_phase(phase, body, first=0, static=0):
        n = count_of[phase]
        for t in range(first, first + DEPTH - 1):
            start_loads(phase, t)

        def one(t):
            when(t + DEPTH - 1 < n, lambda: start_loads(phase, t + DEPTH - 1))
            for c in loads(phase, t):
                c.wait()
            body(t)
        for t in range(first, static):
            one(t)
        loop(max(first, static), n, one)

    barrier = pltpu.get_barrier_semaphore()
    for other in [partner] + near:
        pl.semaphore_signal(barrier, inc=1, device_id=(other,), device_id_type=MESH)
    for t in range(DEPTH):
        own_load(1, t).start()
    pl.semaphore_wait(barrier, 4)

    for t in range(DEPTH):
        early_copy(t).start()
    for t in range(DEPTH):
        own_load(1, t).wait()
        early_copy(t).wait_recv()
        p, k, j = decode(1, t)

        def fn(i, rows):
            sb[4 * p + j, rows, :] = chip_sum(t, i, early)
        slabs(fn)
        s1_one(p, j).start()
        if t == 0:
            for u in range(DEPTH, 12):
                partner_copy(1, u).start()
    loop(12, 48, lambda t: partner_copy(1, t).start())

    def phase1(t):
        p, k, j = decode(1, t)
        g = 3 * k + p
        if not isinstance(t, int):
            when((t >= 24) & (j == 0), lambda: left(g, 4))
        slot = t % DEPTH

        def fn(i, rows):
            sb[4 * (g % GROUPS) + j, rows, :] = chip_sum(slot, i)
        slabs(fn)
        if isinstance(t, int):
            s1_one(p, j).start()
        else:
            when(j == 3, lambda: s1_copy(p, k).start())

    def phase2(t):
        p, k, j = decode(2, t)
        g = 3 * k + p
        when((j == 0) & (t < 12), lambda: left(g, 4))
        when((j == 0) & (t >= 12), lambda: left(g, 2))
        slot = t % DEPTH

        def fn(i, rows):
            sb[4 * (g % GROUPS) + j, rows, :] = chip_sum(slot, i) + st1[slot, rows, :]
        slabs(fn)
        when(j == 1, lambda: s2_copy(p, k).start())

    def phase3(t):
        p, k, _ = decode(3, t)
        when(t < 6, lambda: left(t, 2))
        when(t >= 6, lambda: left(t, 1))
        slot = t % DEPTH

        def fn(i, rows):
            sb[4 * (t % GROUPS), rows, :] = chip_sum(slot, i) + st1[slot, rows, :] + st2[slot, rows, :]
        slabs(fn)
        s3_copy(p, k).start()

    def early_sum(t):
        return 4 * (t // 3) + 1 + t % 3

    def phase4(t):
        slot = t % DEPTH

        def fn(i, rows):
            sb[early_sum(t), rows, :] = chip_sum(slot, i) + st1[slot, rows, :] + st2[slot, rows, :]
        slabs(fn)

    run_phase(1, phase1, DEPTH, 12)
    for phase in (2, 3, 4):
        loop(0, count_of[phase], lambda t, phase=phase: partner_copy(phase, t).start())
    rows_here(48, 48, LATE).wait_recv()

    pairs = ((w_in, w), (m_in, m), (v_in, v), (mask_in, mask), (lr_in, lr))
    states = [pltpu.make_async_copy(a, b, ld.at[i]) for i, (a, b) in enumerate(pairs)]
    for c in states:
        c.start()
    run_phase(2, phase2)
    for c in states:
        c.wait()
    rows_here(DEPTH, 96 - DEPTH, LATE).wait_send()
    remote(early, early, psend, precv.at[0], partner).wait_send()
    run_phase(3, phase3)
    run_phase(4, phase4)

    acc[...] = jnp.zeros_like(acc)

    def finish(t, skip):
        s3_copy(t % 3, t // 3).wait_recv()

        def fn(i, rows):
            g = (sb[early_sum(t), rows, :] + r3[t, rows, :]) * (1.0 / NDEV)
            r3[t, rows, :] = g
            sq = g * g
            if skip:
                row = lax.broadcasted_iota(jnp.int32, (SLAB, LANES), 0) + i * SLAB
                sq = jnp.where(row < skip, 0.0, sq)
            acc[...] += jnp.sum(sq.reshape(SLAB // 8, 8, LANES), axis=0)
        slabs(fn)

    loop(0, 11, lambda t: finish(t, 0))
    finish(11, 4)

    nrm[me] = acc[...]

    def norm_copy(i):
        return remote(acc, nrm.at[me], ns, nr, lax.rem(me + i, NDEV))

    others = nrm.at[pl.ds(0, NDEV - 1)]
    all_norms = remote(others, others, ns, nr, partner)
    loop(1, NDEV, lambda i: norm_copy(i).start())
    for g in range(6, 12):
        left(g, 1)
    all_norms.wait_recv()
    total = nrm[0]
    for i in range(1, NDEV):
        total = total + nrm[i]
    norm = jnp.sqrt(jnp.sum(total, keepdims=True))
    norm_out[...] = jnp.broadcast_to(norm, norm_out.shape)
    clip = jnp.minimum(1.0, 1.0 / (norm + CLIP_EPS))
    rate = lr[...].reshape(1, 1)

    def block_of(p, n):
        block = me
        for bit in range(3):
            if (n >> bit) & 1:
                block = block + step_of(me, (p + bit) % 3)
        return block

    def end_of(p, k):
        return min(AG_UNITS * (4 * p + k), UNITS)

    def place(p, n, k0, k1):
        return out.at[pl.ds(block_of(p, n) * UNITS + end_of(p, k0), end_of(p, k1) - end_of(p, k0))]

    def ir_index(p, n, k0):
        return 21 + p if (n == 7 and k0) else 3 * (n - 1) + p

    def ici(p, n, hop, k0, k1):
        here = place(p, n, k0, k1)
        return remote(here, here, is_, ir.at[ir_index(p, n | (1 << hop), k0)], near[(p + hop) % 3])

    def arrival(p, n, k0=0, k1=4):
        here = place(p, n, k0, k1)
        return remote(here, here, is_, ir.at[ir_index(p, n, k0)], partner)

    def die(here):
        return remote(here, here, ds_, dr, partner)

    def update(p, k):
        t = 3 * k + p
        q = 4 * p + k
        short = q == CHUNKS - 1

        def slab(row0, n):
            rows = pl.ds(row0 + q * CR, n)
            src = pl.ds(row0 + 4, n) if short else pl.ds(row0, n)
            w_new, m_new, v_new = adam_slab(rate, clip, r3[t, src, :], w[rows, :], m[rows, :], v[rows, :], mask[rows, :])
            w[rows, :] = w_new
            m[rows, :] = m_new
            v[rows, :] = v_new
            return w_new.astype(jnp.bfloat16).reshape(n // 4, 4, LANES)

        base = me * UNITS + q * AG_UNITS
        if short:
            for i in range(0, CR, SLAB):
                n = min(SLAB, ROWS - q * CR - i)
                out[pl.ds(base + i // 4, n // 4)] = slab(i, n)
        else:
            def one(i, _):
                out[pl.ds(base + i * (SLAB // 4), SLAB // 4)] = slab(pl.multiple_of(i * SLAB, SLAB), SLAB)
                return 0
            lax.fori_loop(0, NSLAB, one, 0)

    for p in range(3):
        update(p, 0)
        for hop in range(3):
            ici(p, 0, hop, 0, 1).start()
    for k in range(1, 4):
        for p in range(3):
            update(p, k)
            ici(p, 0, 0, k, k + 1).start()
    for hop in (1, 2):
        for p in range(3):
            ici(p, 0, hop, 1, 4).start()
    die(out.at[pl.ds(me * UNITS, UNITS)]).start()
    all_norms.wait_send()

    def pass_on(n, hops):
        for p in range(3):
            arrival(p, n).wait_recv()
            for hop in hops:
                if n | (1 << hop) == 7:
                    ici(p, n, hop, 0, 3).start()
                    ici(p, n, hop, 3, 4).start()
                else:
                    ici(p, n, hop, 0, 4).start()
            die(place(p, n, 0, 4)).start()

    pass_on(1, (1, 2))
    pass_on(2, (2,))
    pass_on(3, (2,))
    pass_on(4, ())
    pass_on(5, ())
    pass_on(6, ())
    for k0, k1 in ((0, 3), (3, 4)):
        for p in range(3):
            arrival(p, 7, k0, k1).wait_recv()
            die(place(p, 7, k0, k1)).start()
    sends = out.at[pl.ds(0, 7 * UNITS)]
    remote(sends, sends, is_, ir.at[0], partner).wait_send()
    half = out.at[pl.ds(0, 8 * UNITS)]
    die(half).wait_send()
    die(half).wait_recv()


def step(lr, grad, w, m, v, mask):
    f32, bf16 = jnp.float32, jnp.bfloat16
    dma = pltpu.SemaphoreType.DMA
    flat = lambda a: pltpu.with_memory_space_constraint(a.reshape(ROWS, LANES), pltpu.HBM)
    hbm = pl.BlockSpec(memory_space=pl.ANY)
    vmem = pl.BlockSpec(memory_space=pltpu.VMEM)
    state = pltpu.VMEM((ROWS, LANES), f32)
    return pl.pallas_call(
        step_kernel,
        out_shape=(
            state, state, state, pltpu.VMEM((8, LANES), f32),
            pltpu.VMEM((NDEV * UNITS, 4, LANES), bf16),
            pltpu.HBM((96, 1, CW), bf16), pltpu.HBM((48, CR, LANES), f32), pltpu.HBM((24, CR, LANES), f32),
        ),
        in_specs=[hbm] * 6,
        out_specs=(vmem, vmem, vmem, vmem, vmem, hbm, hbm, hbm),
        scratch_shapes=[
            pltpu.VMEM((1,), f32),
            pltpu.VMEM((DEPTH, 1, CW), bf16),
            pltpu.VMEM((DEPTH, 1, CW), bf16),
            pltpu.VMEM((DEPTH, CR, LANES), f32),
            pltpu.VMEM((DEPTH, CR, LANES), f32),
            pltpu.VMEM((DEPTH, 1, CW), bf16),
            pltpu.VMEM((ROWS, LANES), jnp.int32),
            pltpu.VMEM((4 * GROUPS, CR, LANES), f32),
            pltpu.VMEM((12, CR, LANES), f32),
            pltpu.VMEM((8, LANES), f32),
            pltpu.VMEM((NDEV, 8, LANES), f32),
            dma(()), dma((LATE + 1 + DEPTH,)), dma((GROUPS,)),
            dma((12,)), dma((12,)), dma((12,)),
            dma(()), dma(()),
            dma((DEPTH,)), dma((DEPTH,)), dma((DEPTH,)), dma((DEPTH,)),
            dma((5,)),
            dma(()), dma((24,)), dma(()), dma(()),
        ],
        compiler_params=pltpu.CompilerParams(collective_id=0, has_side_effects=True, vmem_limit_bytes=22 * 1024 * 1024),
        name='step',
    )(lr, grad, flat(w), flat(m), flat(v), flat(mask))


PUBLISH_PIECES = 8


def publish_kernel(p_in, w_in, m_in, v_in, n_in, p_out, w_out, m_out, v_out, n_out, big, small):
    size = NDEV * UNITS // PUBLISH_PIECES
    copies = [pltpu.make_async_copy(p_in.at[pl.ds(i * size, size)], p_out.at[pl.ds(i * size, size)], big.at[i]) for i in range(PUBLISH_PIECES)]
    copies += [pltpu.make_async_copy(a, b, small.at[i]) for i, (a, b) in enumerate(((w_in, w_out), (m_in, m_out), (v_in, v_out)))]
    for c in copies:
        c.start()
    n_out[...] = n_in[0, 0:1]
    for c in copies:
        c.wait()


def publish(arrays, norm):
    dma = pltpu.SemaphoreType.DMA
    vmem = pl.BlockSpec(memory_space=pltpu.VMEM)
    hbm = pl.BlockSpec(memory_space=pl.ANY)
    arrays = [pltpu.with_memory_space_constraint(a, pltpu.VMEM) for a in arrays]
    norm = pltpu.with_memory_space_constraint(norm, pltpu.VMEM)
    return pl.pallas_call(
        publish_kernel,
        out_shape=[jax.ShapeDtypeStruct(a.shape, a.dtype) for a in arrays] + [jax.ShapeDtypeStruct((1,), jnp.float32)],
        in_specs=[vmem] * 5,
        out_specs=[hbm] * 4 + [vmem],
        scratch_shapes=[dma((PUBLISH_PIECES,)), dma((3,))],
        compiler_params=pltpu.CompilerParams(vmem_limit_bytes=1024 * 1024),
        name='publish',
    )(*arrays, norm)


def solution(mesh):
    def local_step(grad_row, master, mom_first, mom_second, decay_mask, learn_rate):
        w, m, v, norm, params, *_ = step(learn_rate, grad_row, master, mom_first, mom_second, decay_mask)
        params, w, m, v, norm = publish([params, w, m, v], norm)
        return params.reshape(-1), w.reshape(-1), m.reshape(-1), v.reshape(-1), norm

    return jax.shard_map(local_step, mesh=mesh, in_specs=(P('dp', None), P('dp'), P('dp'), P('dp'), P('dp'), P()), out_specs=(P(), P('dp'), P('dp'), P('dp'), P()), check_vma=False)
```

```python
import jax
import jax.numpy as jnp
from jax import lax
from jax.experimental import pallas as pl
from jax.experimental.pallas import tpu as pltpu
from jax.sharding import PartitionSpec as P

BETA_FIRST = 0.9
BETA_SECOND = 0.95
ADAM_EPS = 1e-8
CLIP_EPS = 1e-6
WEIGHT_DECAY = 0.1
ADAM_STEP = 10

NDEV = 16
LANES = 128
ROWS = 6908
ROWS_PAD = 6912
CHUNKS = 12
CR = 576
CW = CR * LANES
SLAB = 144
NSLAB = CR // SLAB
DEPTH = 4
GROUPS = 6
UNITS = ROWS // 4
LATE = 12
PIECES = {1: (0, 4), 2: (0, 4), 3: (0, 4), 4: (0, 4), 5: (0, 3, 4), 6: (0, 3, 4), 7: (0, 0.5)}
LATE_FROM = 0.5
AG_UNITS = 144

MESH = pl.DeviceIdType.MESH


def weight(axis):
    return 2 + axis + axis * axis


def step_of(me, axis):
    w = weight(axis)
    return (1 - 2 * ((me // w) % 2)) * w


def chunk_row(q):
    return CR * q - 4 * (q // (CHUNKS - 1))


def end_of(p, k):
    return min(int(AG_UNITS * (4 * p + k)), UNITS)


LATE_UNITS = [end_of(p, 4) - end_of(p, LATE_FROM) for p in range(3)]


def remote(src, dst, ssem, rsem, dev):
    return pltpu.make_async_remote_copy(src_ref=src, dst_ref=dst, send_sem=ssem, recv_sem=rsem, device_id=(dev,), device_id_type=MESH)


def adam_slab(lr, clip, g, w, m, v, mask):
    h = g * clip
    m_new = BETA_FIRST * m + (1.0 - BETA_FIRST) * h
    v_new = BETA_SECOND * v + (1.0 - BETA_SECOND) * h * h
    step_dir = (m_new / (1.0 - BETA_FIRST ** ADAM_STEP)) / (jnp.sqrt(v_new / (1.0 - BETA_SECOND ** ADAM_STEP)) + ADAM_EPS)
    w_new = w - lr * (step_dir + WEIGHT_DECAY * mask.astype(jnp.float32) * w)
    return w_new, m_new, v_new


def step_kernel(lr_in, grad, w_in, m_in, v_in, mask_in, w, m, v, norm_out, out, late0, late1, late2, prow, r1, r2,
                lr, own, par, st1, st2, early, raw, first, mask, sb, r3, acc, nrm,
                fs, fr, psend, precv, sent, s1r, s2r, s3r, ns, nr, lo, lp, l1, l2, ld, le, is_, ir, ds_, dr):
    me = lax.axis_index('dp')
    partner = me + 1 - 2 * (me % 2)
    near = [me + step_of(me, a) for a in range(3)]

    base_of = {1: 0, 2: 48, 3: 72, 4: 84}
    count_of = {1: 48, 2: 24, 3: 12, 4: 12}

    def decode(phase, t):
        if phase == 1:
            if isinstance(t, int) and t < 12:
                return t % 3, 0, t // 3
            return (t // 4) % 3, t // 12, t % 4
        if phase == 2:
            return (t // 2) % 3, t // 6, t % 2
        return t % 3, t // 3, 0

    def where(phase, t):
        p, k, j = decode(phase, t)
        if phase == 1:
            o1, o2, o3 = 1, j % 2, j // 2
        elif phase == 2:
            o1, o2, o3 = 0, 1, j
        else:
            o1, o2, o3 = 0, 0, 1 if phase == 3 else 0
        shift = o1 * step_of(me, p) + o2 * step_of(me, (p + 1) % 3) + o3 * step_of(me, (p + 2) % 3)
        return shift, 4 * p + k

    def grad_slice(block, q):
        start = pl.multiple_of((block * ROWS + chunk_row(q)) * LANES, LANES)
        return grad.at[:, pl.ds(start, CW)]

    core = me % 2

    def first_load(p, c):
        shift, q = where(1, p)
        stage = par if c else own
        return pltpu.make_async_copy(grad_slice(me - core + c + shift, q), stage.at[p], (lp if c else lo).at[p])

    def first_copy(p, c):
        dev = me - core + c + step_of(me, p)
        return remote(raw.at[p, c], first.at[p, core], fs, fr, dev)

    def all_first(here):
        return remote(here, here, fs, fr, partner)

    def early_copy():
        shift, q = where(1, 3)
        return remote(grad_slice(partner + shift, q), early, psend, precv.at[LATE + 1], partner)

    def partner_copy(phase, t):
        shift, q = where(phase, t)
        group = t // 4 if phase == 1 else LATE
        return remote(grad_slice(partner + shift, q), prow.at[base_of[phase] + t], psend, precv.at[group], partner)

    def rows_here(first, count, group):
        rows = prow.at[pl.ds(first, count)]
        return remote(rows, rows, psend, precv.at[group], partner)

    def own_load(phase, t):
        shift, q = where(phase, t)
        slot = t % DEPTH
        return pltpu.make_async_copy(grad_slice(me + shift, q), own.at[slot], lo.at[slot])

    def slots(g, count):
        return sb.at[pl.ds(4 * (g % GROUPS), count)]

    def s1_one(p, j):
        return remote(sb.at[4 * p + j], r1.at[16 * p + j], sent.at[p], s1r.at[4 * p], me + step_of(me, p))

    def s1_copy(p, k):
        g = 3 * k + p
        return remote(slots(g, 4), r1.at[pl.ds((4 * p + k) * 4, 4)], sent.at[g % GROUPS], s1r.at[4 * p + k], me + step_of(me, p))

    def s2_copy(p, k):
        g = 3 * k + p
        return remote(slots(g, 2), r2.at[pl.ds((4 * p + k) * 2, 2)], sent.at[g % GROUPS], s2r.at[4 * p + k], me + step_of(me, (p + 1) % 3))

    def s3_copy(p, k):
        g = 3 * k + p
        return remote(sb.at[4 * (g % GROUPS)], r3.at[g], sent.at[g % GROUPS], s3r.at[g], me + step_of(me, (p + 2) % 3))

    def s1_three(p):
        here = r1.at[pl.ds(16 * p + 1, 3)]
        return remote(here, here, sent.at[p], s1r.at[4 * p], partner)

    def left(g, count):
        here = slots(g, count)
        remote(here, here, sent.at[g % GROUPS], s1r.at[0], partner).wait_send()

    def left_three(g):
        here = sb.at[pl.ds(4 * (g % GROUPS) + 1, 3)]
        remote(here, here, sent.at[g % GROUPS], s1r.at[0], partner).wait_send()

    def sources(phase, t):
        p, k, j = decode(phase, t)
        q = 4 * p + k
        if phase == 2:
            return 4 * q + 2 * j + 1, None
        if phase == 3:
            return 4 * q + 2, 2 * q + 1
        return 4 * q, 2 * q

    def loads(phase, t):
        slot = t % DEPTH
        copies = [own_load(phase, t), pltpu.make_async_copy(prow.at[base_of[phase] + t], par.at[slot], lp.at[slot])]
        if phase > 1:
            i1, i2 = sources(phase, t)
            if not (phase == 4 and isinstance(t, int) and t < 3):
                copies.append(pltpu.make_async_copy(r1.at[i1], st1.at[slot], l1.at[slot]))
            if phase > 2:
                copies.append(pltpu.make_async_copy(r2.at[i2], st2.at[slot], l2.at[slot]))
        return copies

    def when(cond, fn):
        if isinstance(cond, bool):
            if cond:
                fn()
        else:
            pl.when(cond)(fn)

    def start_loads(phase, t):
        p, k, j = decode(phase, t)
        if phase == 1:
            when(t % 4 == 0, lambda: rows_here(t, 4, t // 4).wait_recv())
        elif phase == 2:
            when((j == 0) & (t < 6), lambda: s1_three(p).wait_recv())
            when((j == 0) & (t >= 6), lambda: s1_copy(p, k).wait_recv())
        elif phase == 3:
            s2_copy(p, k).wait_recv()
        for c in loads(phase, t):
            c.start()

    def slab_cols(i):
        return pl.ds(pl.multiple_of(i * (SLAB * LANES), SLAB * LANES), SLAB * LANES)

    def chip_sum(slot, i, other=None):
        theirs = par[slot, :, slab_cols(i)] if other is None else other[:, slab_cols(i)]
        total = own[slot, :, slab_cols(i)].astype(jnp.float32) + theirs.astype(jnp.float32)
        return total.reshape(SLAB, LANES)

    def slabs(fn):
        def one(i, _):
            fn(i, pl.ds(pl.multiple_of(i * SLAB, SLAB), SLAB))
            return 0
        lax.fori_loop(0, NSLAB, one, 0)

    def loop(lo_t, hi_t, fn):
        def one(t, _):
            fn(t)
            return 0
        lax.fori_loop(lo_t, hi_t, one, 0)

    def run_phase(phase, body, first=0, static=0):
        n = count_of[phase]
        for t in range(first, first + DEPTH - 1):
            start_loads(phase, t)

        def one(t):
            when(t + DEPTH - 1 < n, lambda: start_loads(phase, t + DEPTH - 1))
            for c in loads(phase, t):
                c.wait()
            body(t)
        for t in range(first, static):
            one(t)
        loop(max(first, static), n, one)

    barrier = pltpu.get_barrier_semaphore()
    for other in [partner] + near + [n + partner - me for n in near]:
        pl.semaphore_signal(barrier, inc=1, device_id=(other,), device_id_type=MESH)
    for p in range(3):
        for c in range(2):
            first_load(p, c).start()
    own_load(1, 3).start()
    for p in range(3):
        for c in range(2):
            first_load(p, c).wait()
            stage = par if c else own

            def fn(i, rows):
                mine = stage[p, :, slab_cols(i)].astype(jnp.float32).reshape(SLAB, LANES)
                raw[p, c, rows, :] = mine.astype(jnp.bfloat16)
            slabs(fn)
        if p == 0:
            pl.semaphore_wait(barrier, 7)
        for c in range(2):
            first_copy(p, c).start()
        if p == 0:
            early_copy().start()
    for u in range(4, 12):
        partner_copy(1, u).start()
    own_load(1, 3).wait()
    early_copy().wait_recv()

    def fn(i, rows):
        sb[1, rows, :] = chip_sum(3, i, early)
    slabs(fn)
    s1_one(0, 1).start()
    loop(12, 48, lambda t: partner_copy(1, t).start())

    def phase1(t):
        p, k, j = decode(1, t)
        g = 3 * k + p
        if not isinstance(t, int):
            when((t >= 24) & (t < 36) & (j == 0), lambda: left_three(g))
            when((t >= 36) & (j == 0), lambda: left(g, 4))
        slot = t % DEPTH

        def fn(i, rows):
            sb[4 * (g % GROUPS) + j, rows, :] = chip_sum(slot, i)
        slabs(fn)
        if isinstance(t, int):
            s1_one(p, j).start()
        else:
            when(j == 3, lambda: s1_copy(p, k).start())

    def phase2(t):
        p, k, j = decode(2, t)
        g = 3 * k + p
        when((j == 0) & (t < 12), lambda: left(g, 4))
        when((j == 0) & (t >= 12), lambda: left(g, 2))
        slot = t % DEPTH

        def fn(i, rows):
            sb[4 * (g % GROUPS) + j, rows, :] = chip_sum(slot, i) + st1[slot, rows, :]
        slabs(fn)
        when(j == 1, lambda: s2_copy(p, k).start())

    def phase3(t):
        p, k, _ = decode(3, t)
        when(t < 6, lambda: left(t, 2))
        when(t >= 6, lambda: left(t, 1))
        slot = t % DEPTH

        def fn(i, rows):
            sb[4 * (t % GROUPS), rows, :] = chip_sum(slot, i) + st1[slot, rows, :] + st2[slot, rows, :]
        slabs(fn)
        s3_copy(p, k).start()

    def early_sum(t):
        return 4 * (t // 3) + 1 + t % 3

    def phase4(t):
        slot = t % DEPTH

        def fn(i, rows):
            if isinstance(t, int):
                r1_part = first[t, 0, rows, :].astype(jnp.float32) + first[t, 1, rows, :].astype(jnp.float32)
            else:
                r1_part = st1[slot, rows, :]
            sb[early_sum(t), rows, :] = chip_sum(slot, i) + r1_part + st2[slot, rows, :]
        slabs(fn)

    run_phase(1, phase1, DEPTH, 12)
    for phase in (2, 3, 4):
        loop(0, count_of[phase], lambda t, phase=phase: partner_copy(phase, t).start())
    rows_here(48, 48, LATE).wait_recv()

    pairs = ((w_in, w), (m_in, m), (v_in, v), (mask_in, mask), (lr_in, lr))
    states = [pltpu.make_async_copy(a, b, ld.at[i]) for i, (a, b) in enumerate(pairs)]
    for c in states:
        c.start()
    run_phase(2, phase2)
    for c in states:
        c.wait()
    rows_here(4, 92, LATE).wait_send()
    early_copy().wait_send()
    all_first(raw).wait_send()
    all_first(first).wait_recv()
    run_phase(3, phase3)
    run_phase(4, phase4, 0, 3)

    acc[...] = jnp.zeros_like(acc)

    def finish(t, skip):
        s3_copy(t % 3, t // 3).wait_recv()

        def fn(i, rows):
            g = (sb[early_sum(t), rows, :] + r3[t, rows, :]) * (1.0 / NDEV)
            r3[t, rows, :] = g
            sq = g * g
            if skip:
                row = lax.broadcasted_iota(jnp.int32, (SLAB, LANES), 0) + i * SLAB
                sq = jnp.where(row < skip, 0.0, sq)
            acc[...] += jnp.sum(sq.reshape(SLAB // 8, 8, LANES), axis=0)
        slabs(fn)

    loop(0, 11, lambda t: finish(t, 0))
    finish(11, 4)

    nrm[me] = acc[...]

    def norm_copy(i):
        return remote(acc, nrm.at[me], ns, nr, i)

    others = nrm.at[pl.ds(0, NDEV - 1)]
    all_norms = remote(others, others, ns, nr, partner)
    far = sum(step_of(me, a) for a in range(3))
    hops = [step_of(me, a) for a in range(3)]
    for shift in [far] + [far - h for h in hops] + hops:
        for dev in (me + shift, partner + shift):
            norm_copy(dev).start()
    norm_copy(partner).start()
    for g in range(6, 12):
        left(g, 1)
    all_norms.wait_recv()
    total = nrm[0]
    for i in range(1, NDEV):
        total = total + nrm[i]
    norm = jnp.sqrt(jnp.sum(total, keepdims=True))
    norm_out[...] = jnp.broadcast_to(norm, norm_out.shape)
    clip = jnp.minimum(1.0, 1.0 / (norm + CLIP_EPS))
    rate = lr[...]

    def block_of(p, n):
        block = me
        for bit in range(3):
            if (n >> bit) & 1:
                block = block + step_of(me, (p + bit) % 3)
        return block

    def place(p, n, k0, k1):
        return out.at[pl.ds(block_of(p, n) * UNITS + end_of(p, k0), end_of(p, k1) - end_of(p, k0))]

    def late_copy(p):
        return pltpu.make_async_copy(place(p, 3, LATE_FROM, 4), (late0, late1, late2)[p], le.at[p])

    def ir_index(p, n, k0):
        before = sum(len(PIECES[b]) - 1 for b in range(1, n))
        piece = sum(1 for edge in PIECES[n][1:] if edge <= k0)
        return 3 * (before + piece) + p

    def ici(p, n, hop, k0, k1):
        here = place(p, n, k0, k1)
        return remote(here, here, is_, ir.at[ir_index(p, n | (1 << hop), k0)], near[(p + hop) % 3])

    def arrival(p, n, k0, k1):
        here = place(p, n, k0, k1)
        return remote(here, here, is_, ir.at[ir_index(p, n, k0)], partner)

    def die(here):
        return remote(here, here, ds_, dr, partner)

    def update(p, k, lo_slab=0, hi_slab=NSLAB):
        t = 3 * k + p
        q = 4 * p + k
        short = q == CHUNKS - 1

        def slab(row0, n):
            rows = pl.ds(row0 + q * CR, n)
            src = pl.ds(row0 + 4, n) if short else pl.ds(row0, n)
            w_new, m_new, v_new = adam_slab(rate, clip, r3[t, src, :], w[rows, :], m[rows, :], v[rows, :], mask[rows, :])
            w[rows, :] = w_new
            m[rows, :] = m_new
            v[rows, :] = v_new
            return w_new.astype(jnp.bfloat16).reshape(n // 4, 4, LANES)

        base = me * UNITS + q * AG_UNITS
        if short:
            for i in range(0, CR, SLAB):
                n = min(SLAB, ROWS - q * CR - i)
                out[pl.ds(base + i // 4, n // 4)] = slab(i, n)
        else:
            def one(i, _):
                out[pl.ds(base + i * (SLAB // 4), SLAB // 4)] = slab(pl.multiple_of(i * SLAB, SLAB), SLAB)
                return 0
            lax.fori_loop(lo_slab, hi_slab, one, 0)

    for p in range(3):
        for k0, k1 in ((0, 0.25), (0.25, 1)) if p == 0 else ((0, 1),):
            update(p, 0, int(k0 * NSLAB), int(k1 * NSLAB))
            for hop in range(3):
                ici(p, 0, hop, k0, k1).start()
    for k in range(1, 4):
        for p in range(3):
            update(p, k)
            ici(p, 0, 0, k, k + 1).start()
    for hop in (1, 2):
        for p in range(3):
            ici(p, 0, hop, 1, 4).start()
    die(out.at[pl.ds(me * UNITS, UNITS)]).start()
    all_norms.wait_send()

    def pass_on(n, hops):
        for k0, k1 in zip(PIECES[n], PIECES[n][1:]):
            for p in range(3):
                arrival(p, n, k0, k1).wait_recv()
                for hop in hops:
                    last = min(k1, PIECES[n | (1 << hop)][-1])
                    edges = [k0] + [e for e in PIECES[n | (1 << hop)] if k0 < e < last] + [last]
                    for e0, e1 in zip(edges, edges[1:]):
                        ici(p, n, hop, e0, e1).start()
                if n == 3:
                    late_copy(p).start()
                die(place(p, n, k0, k1)).start()

    pass_on(1, (1, 2))
    pass_on(2, (2,))
    pass_on(3, (2,))
    pass_on(4, ())
    pass_on(5, ())
    pass_on(6, ())
    pass_on(7, ())
    sends = out.at[pl.ds(0, 7 * UNITS - sum(LATE_UNITS))]
    remote(sends, sends, is_, ir.at[0], partner).wait_send()
    half = out.at[pl.ds(0, 8 * UNITS - sum(LATE_UNITS))]
    die(half).wait_send()
    die(half).wait_recv()
    for p in range(3):
        late_copy(p).wait()


def step(lr, grad, w, m, v, mask):
    f32, bf16 = jnp.float32, jnp.bfloat16
    dma = pltpu.SemaphoreType.DMA
    flat = lambda a: pltpu.with_memory_space_constraint(a.reshape(ROWS, LANES), pltpu.HBM)
    hbm = pl.BlockSpec(memory_space=pl.ANY)
    vmem = pl.BlockSpec(memory_space=pltpu.VMEM)
    state = pltpu.VMEM((ROWS, LANES), f32)
    return pl.pallas_call(
        step_kernel,
        out_shape=(
            state, state, state, pltpu.VMEM((8, LANES), f32),
            pltpu.VMEM((NDEV * UNITS, 4, LANES), bf16),
            *[pltpu.HBM((n, 4, LANES), bf16) for n in LATE_UNITS],
            pltpu.HBM((96, 1, CW), bf16), pltpu.HBM((48, CR, LANES), f32), pltpu.HBM((24, CR, LANES), f32),
        ),
        in_specs=[hbm] * 6,
        out_specs=(vmem,) * 5 + (hbm,) * 6,
        scratch_shapes=[
            pltpu.VMEM((1, 1), f32),
            pltpu.VMEM((DEPTH, 1, CW), bf16),
            pltpu.VMEM((DEPTH, 1, CW), bf16),
            pltpu.VMEM((DEPTH, CR, LANES), f32),
            pltpu.VMEM((DEPTH, CR, LANES), f32),
            pltpu.VMEM((1, CW), bf16),
            pltpu.VMEM((3, 2, CR, LANES), bf16),
            pltpu.VMEM((3, 2, CR, LANES), bf16),
            pltpu.VMEM((ROWS, LANES), jnp.int32),
            pltpu.VMEM((4 * GROUPS, CR, LANES), f32),
            pltpu.VMEM((12, CR, LANES), f32),
            pltpu.VMEM((8, LANES), f32),
            pltpu.VMEM((NDEV, 8, LANES), f32),
            dma(()), dma(()),
            dma(()), dma((LATE + 2,)), dma((GROUPS,)),
            dma((12,)), dma((12,)), dma((12,)),
            dma(()), dma(()),
            dma((DEPTH,)), dma((DEPTH,)), dma((DEPTH,)), dma((DEPTH,)),
            dma((5,)), dma((3,)),
            dma(()), dma((3 * sum(len(e) - 1 for e in PIECES.values()),)), dma(()), dma(()),
        ],
        compiler_params=pltpu.CompilerParams(collective_id=0, has_side_effects=True, vmem_limit_bytes=22 * 1024 * 1024),
        name='step',
    )(lr.reshape(1, 1), grad, flat(w), flat(m), flat(v), flat(mask))


def publish_kernel(p_in, w_in, m_in, v_in, n_in, p_out, w_out, m_out, v_out, n_out, big, small):
    me = lax.axis_index('dp')
    base = me - me % 2
    late = late_blocks()
    spans = []
    for n in range(7):
        block = base
        for bit in range(3):
            if (n >> bit) & 1:
                block = block + step_of(me, bit)
        spans.append((block * UNITS, 2 * UNITS))
    for c in range(2):
        for p in range(3):
            spans.append(((late + c) * UNITS + end_of(p, 0), end_of(p, LATE_FROM) - end_of(p, 0)))
    copies = [pltpu.make_async_copy(p_in.at[pl.ds(a, n)], p_out.at[pl.ds(a, n)], big.at[i]) for i, (a, n) in enumerate(spans)]
    copies += [pltpu.make_async_copy(a, b, small.at[i]) for i, (a, b) in enumerate(((w_in, w_out), (m_in, m_out), (v_in, v_out)))]
    for c in copies:
        c.start()
    n_out[...] = n_in[0, 0:1]
    for c in copies:
        c.wait()


def publish(arrays, norm):
    dma = pltpu.SemaphoreType.DMA
    vmem = pl.BlockSpec(memory_space=pltpu.VMEM)
    hbm = pl.BlockSpec(memory_space=pl.ANY)
    arrays = [pltpu.with_memory_space_constraint(a, pltpu.VMEM) for a in arrays]
    norm = pltpu.with_memory_space_constraint(norm, pltpu.VMEM)
    return pl.pallas_call(
        publish_kernel,
        out_shape=[jax.ShapeDtypeStruct(a.shape, a.dtype) for a in arrays] + [jax.ShapeDtypeStruct((1,), jnp.float32)],
        in_specs=[vmem] * 5,
        out_specs=[hbm] * 4 + [vmem],
        scratch_shapes=[dma((13,)), dma((3,))],
        compiler_params=pltpu.CompilerParams(vmem_limit_bytes=1024 * 1024),
        cost_estimate=pl.CostEstimate(flops=40_000_000, bytes_accessed=40_000_000, transcendentals=0),
        name='publish',
    )(*arrays, norm)


def late_blocks():
    me = lax.axis_index('dp')
    return me - me % 2 + step_of(me, 0) + step_of(me, 1) + step_of(me, 2)


def place_late(params, pieces, other):
    def kernel(p_in, piece0, piece1, piece2, p_out, sem):
        core = lax.axis_index('dp') % 2
        block = late_blocks() + (1 - core if other else core)
        copies = []
        for p, piece in enumerate((piece0, piece1, piece2)):
            here = p_out.at[pl.ds(block * UNITS + end_of(p, LATE_FROM), LATE_UNITS[p])]
            copies.append(pltpu.make_async_copy(piece, here, sem.at[p]))
        for c in copies:
            c.start()
        for c in copies:
            c.wait()

    hbm = pl.BlockSpec(memory_space=pl.ANY)
    vmem = pl.BlockSpec(memory_space=pltpu.VMEM)
    return pl.pallas_call(
        kernel,
        out_shape=jax.ShapeDtypeStruct(params.shape, params.dtype),
        in_specs=[hbm] + [vmem] * 3,
        out_specs=hbm,
        scratch_shapes=[pltpu.SemaphoreType.DMA((3,))],
        input_output_aliases={0: 0},
        compiler_params=pltpu.CompilerParams(vmem_limit_bytes=4 * 1024 * 1024),
        cost_estimate=pl.CostEstimate(flops=4_000_000, bytes_accessed=4_000_000, transcendentals=0),
        name='place_other' if other else 'place_own',
    )(params, *pieces)


def solution(mesh):
    def local_step(grad_row, master, mom_first, mom_second, decay_mask, learn_rate):
        w, m, v, norm, params, late0, late1, late2, *_ = step(learn_rate, grad_row, master, mom_first, mom_second, decay_mask)
        pieces = []
        for p, late in enumerate((late0, late1, late2)):
            stride = weight((p + 2) % 3)
            pieces.append(lax.ppermute(late, 'dp', [(d, d ^ stride) for d in range(NDEV)]))
        params, w, m, v, norm = publish([params, w, m, v], norm)
        *pieces, norm = lax.optimization_barrier((*pieces, norm))
        others = [lax.ppermute(piece, 'dp', [(d, d ^ 1) for d in range(NDEV)]) for piece in pieces]
        params = place_late(params, pieces, False)
        params = place_late(params, others, True)
        return params.reshape(-1), w.reshape(-1), m.reshape(-1), v.reshape(-1), norm

    return jax.shard_map(local_step, mesh=mesh, in_specs=(P('dp', None), P('dp'), P('dp'), P('dp'), P('dp'), P()), out_specs=(P(), P('dp'), P('dp'), P('dp'), P()), check_vma=False)
```

```python
import jax
import jax.numpy as jnp
from jax import lax
from jax.experimental import pallas as pl
from jax.experimental.pallas import tpu as pltpu
from jax.sharding import PartitionSpec as P

BETA_FIRST = 0.9
BETA_SECOND = 0.95
ADAM_EPS = 1e-8
CLIP_EPS = 1e-6
WEIGHT_DECAY = 0.1
ADAM_STEP = 10

NDEV = 16
LANES = 128
ROWS = 6908
ROWS_PAD = 6912
CHUNKS = 12
CR = 576
CW = CR * LANES
SLAB = 144
NSLAB = CR // SLAB
DEPTH = 4
GROUPS = 6
UNITS = ROWS // 4
LATE = 12
PIECES = {1: (0, 4), 2: (0, 4), 3: (0, 4), 4: (0, 4), 5: (0, 3, 4), 6: (0, 3, 4), 7: (0, 0.75)}
LATE_FROM = 0.75
AG_UNITS = 144

MESH = pl.DeviceIdType.MESH


def weight(axis):
    return 2 + axis + axis * axis


def step_of(me, axis):
    w = weight(axis)
    return (1 - 2 * ((me // w) % 2)) * w


def chunk_row(q):
    return CR * q - 4 * (q // (CHUNKS - 1))


def end_of(p, k):
    return min(int(AG_UNITS * (4 * p + k)), UNITS)


LATE_UNITS = [end_of(p, 4) - end_of(p, LATE_FROM) for p in range(3)]


def remote(src, dst, ssem, rsem, dev):
    return pltpu.make_async_remote_copy(src_ref=src, dst_ref=dst, send_sem=ssem, recv_sem=rsem, device_id=(dev,), device_id_type=MESH)


def adam_slab(lr, clip, g, w, m, v, mask):
    h = g * clip
    m_new = BETA_FIRST * m + (1.0 - BETA_FIRST) * h
    v_new = BETA_SECOND * v + (1.0 - BETA_SECOND) * h * h
    step_dir = (m_new / (1.0 - BETA_FIRST ** ADAM_STEP)) / (jnp.sqrt(v_new / (1.0 - BETA_SECOND ** ADAM_STEP)) + ADAM_EPS)
    w_new = w - lr * (step_dir + WEIGHT_DECAY * mask.astype(jnp.float32) * w)
    return w_new, m_new, v_new


def step_kernel(lr_in, grad, w_in, m_in, v_in, mask_in, w, m, v, norm_out, out, late0, late1, late2, prow, r1, r2,
                lr, own, par, st1, st2, early, raw, first, mask, sb, r3, acc, nrm,
                fs, fr, psend, precv, sent, s1r, s2r, s3r, ns, nr, lo, lp, l1, l2, ld, le, is_, ir, ds_, dr):
    me = lax.axis_index('dp')
    partner = me + 1 - 2 * (me % 2)
    near = [me + step_of(me, a) for a in range(3)]

    base_of = {1: 0, 2: 48, 3: 72, 4: 84}
    count_of = {1: 48, 2: 24, 3: 12, 4: 12}

    def decode(phase, t):
        if phase == 1:
            if isinstance(t, int) and t < 12:
                return t % 3, 0, t // 3
            return (t // 4) % 3, t // 12, t % 4
        if phase == 2:
            return (t // 2) % 3, t // 6, t % 2
        return t % 3, t // 3, 0

    def where(phase, t):
        p, k, j = decode(phase, t)
        if phase == 1:
            o1, o2, o3 = 1, j % 2, j // 2
        elif phase == 2:
            o1, o2, o3 = 0, 1, j
        else:
            o1, o2, o3 = 0, 0, 1 if phase == 3 else 0
        shift = o1 * step_of(me, p) + o2 * step_of(me, (p + 1) % 3) + o3 * step_of(me, (p + 2) % 3)
        return shift, 4 * p + k

    def grad_slice(block, q):
        start = pl.multiple_of((block * ROWS + chunk_row(q)) * LANES, LANES)
        return grad.at[:, pl.ds(start, CW)]

    core = me % 2

    def first_load(p, c):
        shift, q = where(1, p)
        stage = par if c else own
        return pltpu.make_async_copy(grad_slice(me - core + c + shift, q), stage.at[p], (lp if c else lo).at[p])

    def first_copy(p, c):
        dev = me - core + c + step_of(me, p)
        return remote(raw.at[p, c], first.at[p, core], fs, fr, dev)

    def all_first(here):
        return remote(here, here, fs, fr, partner)

    def early_copy():
        shift, q = where(1, 3)
        return remote(grad_slice(partner + shift, q), early, psend, precv.at[LATE + 1], partner)

    def partner_copy(phase, t):
        shift, q = where(phase, t)
        group = t // 4 if phase == 1 else LATE
        return remote(grad_slice(partner + shift, q), prow.at[base_of[phase] + t], psend, precv.at[group], partner)

    def rows_here(first, count, group):
        rows = prow.at[pl.ds(first, count)]
        return remote(rows, rows, psend, precv.at[group], partner)

    def own_load(phase, t):
        shift, q = where(phase, t)
        slot = t % DEPTH
        return pltpu.make_async_copy(grad_slice(me + shift, q), own.at[slot], lo.at[slot])

    def slots(g, count):
        return sb.at[pl.ds(4 * (g % GROUPS), count)]

    def s1_one(p, j):
        return remote(sb.at[4 * p + j], r1.at[16 * p + j], sent.at[p], s1r.at[0], me + step_of(me, p))

    def s1_copy(p, k):
        g = 3 * k + p
        return remote(slots(g, 4), r1.at[pl.ds((4 * p + k) * 4, 4)], sent.at[g % GROUPS], s1r.at[k], me + step_of(me, p))

    def s2_copy(p, k):
        g = 3 * k + p
        return remote(slots(g, 2), r2.at[pl.ds((4 * p + k) * 2, 2)], sent.at[g % GROUPS], s2r.at[k], me + step_of(me, (p + 1) % 3))

    def s3_copy(p, k):
        g = 3 * k + p
        return remote(sb.at[4 * (g % GROUPS)], r3.at[g], sent.at[g % GROUPS], s3r.at[g], me + step_of(me, (p + 2) % 3))

    def arrived(buf, count, sem):
        here = buf.at[pl.ds(0, count)]
        remote(here, here, sent.at[0], sem, partner).wait_recv()

    def left(g, count):
        here = slots(g, count)
        remote(here, here, sent.at[g % GROUPS], s1r.at[0], partner).wait_send()

    def left_three(g):
        here = sb.at[pl.ds(4 * (g % GROUPS) + 1, 3)]
        remote(here, here, sent.at[g % GROUPS], s1r.at[0], partner).wait_send()

    def sources(phase, t):
        p, k, j = decode(phase, t)
        q = 4 * p + k
        if phase == 2:
            return 4 * q + 2 * j + 1, None
        if phase == 3:
            return 4 * q + 2, 2 * q + 1
        return 4 * q, 2 * q

    def loads(phase, t):
        slot = t % DEPTH
        copies = [own_load(phase, t), pltpu.make_async_copy(prow.at[base_of[phase] + t], par.at[slot], lp.at[slot])]
        if phase > 1:
            i1, i2 = sources(phase, t)
            if not (phase == 4 and isinstance(t, int) and t < 3):
                copies.append(pltpu.make_async_copy(r1.at[i1], st1.at[slot], l1.at[slot]))
            if phase > 2:
                copies.append(pltpu.make_async_copy(r2.at[i2], st2.at[slot], l2.at[slot]))
        return copies

    def when(cond, fn):
        if isinstance(cond, bool):
            if cond:
                fn()
        else:
            pl.when(cond)(fn)

    def start_loads(phase, t):
        p, k, j = decode(phase, t)
        if phase == 1:
            when(t % 4 == 0, lambda: rows_here(t, 4, t // 4).wait_recv())
        elif phase == 2:
            when(t == 0, lambda: arrived(r1, 9, s1r.at[0]))
            when((t % 6 == 0) & (t >= 6), lambda: arrived(r1, 12, s1r.at[k]))
        elif phase == 3:
            when(p == 0, lambda: arrived(r2, 6, s2r.at[k]))
        for c in loads(phase, t):
            c.start()

    def slab_cols(i):
        return pl.ds(pl.multiple_of(i * (SLAB * LANES), SLAB * LANES), SLAB * LANES)

    def chip_sum(slot, i, other=None):
        theirs = par[slot, :, slab_cols(i)] if other is None else other[:, slab_cols(i)]
        total = own[slot, :, slab_cols(i)].astype(jnp.float32) + theirs.astype(jnp.float32)
        return total.reshape(SLAB, LANES)

    def slabs(fn):
        def one(i, _):
            fn(i, pl.ds(pl.multiple_of(i * SLAB, SLAB), SLAB))
            return 0
        lax.fori_loop(0, NSLAB, one, 0)

    def loop(lo_t, hi_t, fn):
        def one(t, _):
            fn(t)
            return 0
        lax.fori_loop(lo_t, hi_t, one, 0)

    def run_phase(phase, body, first=0, static=0):
        n = count_of[phase]
        for t in range(first, first + DEPTH - 1):
            start_loads(phase, t)

        def one(t):
            when(t + DEPTH - 1 < n, lambda: start_loads(phase, t + DEPTH - 1))
            for c in loads(phase, t):
                c.wait()
            body(t)
        for t in range(first, static):
            one(t)
        loop(max(first, static), n, one)

    barrier = pltpu.get_barrier_semaphore()
    for other in [partner] + near + [n + partner - me for n in near]:
        pl.semaphore_signal(barrier, inc=1, device_id=(other,), device_id_type=MESH)
    for p in range(3):
        for c in range(2):
            first_load(p, c).start()
    own_load(1, 3).start()
    for p in range(3):
        for c in range(2):
            first_load(p, c).wait()
            stage = par if c else own

            def fn(i, rows):
                mine = stage[p, :, slab_cols(i)].astype(jnp.float32).reshape(SLAB, LANES)
                raw[p, c, rows, :] = mine.astype(jnp.bfloat16)
            slabs(fn)
            if p == 0 and c == 0:
                pl.semaphore_wait(barrier, 7)
            first_copy(p, c).start()
        if p == 0:
            early_copy().start()
    for u in range(4, 12):
        partner_copy(1, u).start()
    own_load(1, 3).wait()
    early_copy().wait_recv()

    def fn(i, rows):
        sb[1, rows, :] = chip_sum(3, i, early)
    slabs(fn)
    s1_one(0, 1).start()
    loop(12, 48, lambda t: partner_copy(1, t).start())

    def phase1(t):
        p, k, j = decode(1, t)
        g = 3 * k + p
        if not isinstance(t, int):
            when((t >= 24) & (t < 36) & (j == 0), lambda: left_three(g))
            when((t >= 36) & (j == 0), lambda: left(g, 4))
        slot = t % DEPTH

        def fn(i, rows):
            sb[4 * (g % GROUPS) + j, rows, :] = chip_sum(slot, i)
        slabs(fn)
        if isinstance(t, int):
            s1_one(p, j).start()
        else:
            when(j == 3, lambda: s1_copy(p, k).start())

    def phase2(t):
        p, k, j = decode(2, t)
        g = 3 * k + p
        when((j == 0) & (t < 12), lambda: left(g, 4))
        when((j == 0) & (t >= 12), lambda: left(g, 2))
        slot = t % DEPTH

        def fn(i, rows):
            sb[4 * (g % GROUPS) + j, rows, :] = chip_sum(slot, i) + st1[slot, rows, :]
        slabs(fn)
        when(j == 1, lambda: s2_copy(p, k).start())

    def phase3(t):
        p, k, _ = decode(3, t)
        when(t < 6, lambda: left(t, 2))
        when(t >= 6, lambda: left(t, 1))
        slot = t % DEPTH

        def fn(i, rows):
            sb[4 * (t % GROUPS), rows, :] = chip_sum(slot, i) + st1[slot, rows, :] + st2[slot, rows, :]
        slabs(fn)
        s3_copy(p, k).start()

    def early_sum(t):
        return 4 * (t // 3) + 1 + t % 3

    def phase4(t):
        slot = t % DEPTH

        def fn(i, rows):
            if isinstance(t, int):
                r1_part = first[t, 0, rows, :].astype(jnp.float32) + first[t, 1, rows, :].astype(jnp.float32)
            else:
                r1_part = st1[slot, rows, :]
            sb[early_sum(t), rows, :] = chip_sum(slot, i) + r1_part + st2[slot, rows, :]
        slabs(fn)

    run_phase(1, phase1, DEPTH, 12)
    for phase in (2, 3, 4):
        loop(0, count_of[phase], lambda t, phase=phase: partner_copy(phase, t).start())
    rows_here(48, 48, LATE).wait_recv()

    pairs = ((w_in, w), (m_in, m), (v_in, v), (mask_in, mask), (lr_in, lr))
    states = [pltpu.make_async_copy(a, b, ld.at[i]) for i, (a, b) in enumerate(pairs)]
    for c in states:
        c.start()
    run_phase(2, phase2)
    for c in states:
        c.wait()
    rows_here(4, 92, LATE).wait_send()
    early_copy().wait_send()
    all_first(raw).wait_send()
    all_first(first).wait_recv()
    run_phase(3, phase3)
    run_phase(4, phase4, 0, 3)

    acc[...] = jnp.zeros_like(acc)

    def finish(t, skip):
        s3_copy(t % 3, t // 3).wait_recv()

        def fn(i, rows):
            g = (sb[early_sum(t), rows, :] + r3[t, rows, :]) * (1.0 / NDEV)
            r3[t, rows, :] = g
            sq = g * g
            if skip:
                row = lax.broadcasted_iota(jnp.int32, (SLAB, LANES), 0) + i * SLAB
                sq = jnp.where(row < skip, 0.0, sq)
            acc[...] += jnp.sum(sq.reshape(SLAB // 8, 8, LANES), axis=0)
        slabs(fn)

    loop(0, 11, lambda t: finish(t, 0))
    finish(11, 4)

    nrm[me] = acc[...]

    def norm_copy(i):
        return remote(acc, nrm.at[me], ns, nr, i)

    others = nrm.at[pl.ds(0, NDEV - 1)]
    all_norms = remote(others, others, ns, nr, partner)
    far = sum(step_of(me, a) for a in range(3))
    hops = [step_of(me, a) for a in range(3)]
    for shift in [far] + [far - h for h in hops] + hops:
        for dev in (me + shift, partner + shift):
            norm_copy(dev).start()
    norm_copy(partner).start()
    for g in range(6, 12):
        left(g, 1)
    all_norms.wait_recv()
    total = nrm[0]
    for i in range(1, NDEV):
        total = total + nrm[i]
    norm = jnp.sqrt(jnp.sum(total, keepdims=True))
    norm_out[...] = jnp.broadcast_to(norm, norm_out.shape)
    clip = jnp.minimum(1.0, 1.0 / (norm + CLIP_EPS))
    rate = lr[...]

    def block_of(p, n):
        block = me
        for bit in range(3):
            if (n >> bit) & 1:
                block = block + step_of(me, (p + bit) % 3)
        return block

    def place(p, n, k0, k1):
        return out.at[pl.ds(block_of(p, n) * UNITS + end_of(p, k0), end_of(p, k1) - end_of(p, k0))]

    def late_copy(p):
        return pltpu.make_async_copy(place(p, 3, LATE_FROM, 4), (late0, late1, late2)[p], le.at[p])

    def ir_index(p, n, k0):
        before = sum(len(PIECES[b]) - 1 for b in range(1, n))
        piece = sum(1 for edge in PIECES[n][1:] if edge <= k0)
        return 3 * (before + piece) + p

    def ici(p, n, hop, k0, k1):
        here = place(p, n, k0, k1)
        return remote(here, here, is_, ir.at[ir_index(p, n | (1 << hop), k0)], near[(p + hop) % 3])

    def arrival(p, n, k0, k1):
        here = place(p, n, k0, k1)
        return remote(here, here, is_, ir.at[ir_index(p, n, k0)], partner)

    def die(here):
        return remote(here, here, ds_, dr, partner)

    def update(p, k, lo_slab=0, hi_slab=NSLAB):
        t = 3 * k + p
        q = 4 * p + k
        short = q == CHUNKS - 1

        def slab(row0, n):
            rows = pl.ds(row0 + q * CR, n)
            src = pl.ds(row0 + 4, n) if short else pl.ds(row0, n)
            w_new, m_new, v_new = adam_slab(rate, clip, r3[t, src, :], w[rows, :], m[rows, :], v[rows, :], mask[rows, :])
            w[rows, :] = w_new
            m[rows, :] = m_new
            v[rows, :] = v_new
            return w_new.astype(jnp.bfloat16).reshape(n // 4, 4, LANES)

        base = me * UNITS + q * AG_UNITS
        if short:
            for i in range(0, CR, SLAB):
                n = min(SLAB, ROWS - q * CR - i)
                out[pl.ds(base + i // 4, n // 4)] = slab(i, n)
        else:
            def one(i, _):
                out[pl.ds(base + i * (SLAB // 4), SLAB // 4)] = slab(pl.multiple_of(i * SLAB, SLAB), SLAB)
                return 0
            lax.fori_loop(lo_slab, hi_slab, one, 0)

    for p in range(3):
        for k0, k1 in ((0, 0.25), (0.25, 1)) if p == 0 else ((0, 1),):
            update(p, 0, int(k0 * NSLAB), int(k1 * NSLAB))
            for hop in range(3):
                ici(p, 0, hop, k0, k1).start()
    for k in range(1, 4):
        for p in range(3):
            update(p, k)
            ici(p, 0, 0, k, k + 1).start()
    for hop in (1, 2):
        for p in range(3):
            ici(p, 0, hop, 1, 4).start()
    die(out.at[pl.ds(me * UNITS, UNITS)]).start()
    all_norms.wait_send()

    def pass_on(n, hops):
        for k0, k1 in zip(PIECES[n], PIECES[n][1:]):
            for p in range(3):
                arrival(p, n, k0, k1).wait_recv()
                for hop in hops:
                    last = min(k1, PIECES[n | (1 << hop)][-1])
                    edges = [k0] + [e for e in PIECES[n | (1 << hop)] if k0 < e < last] + [last]
                    for e0, e1 in zip(edges, edges[1:]):
                        ici(p, n, hop, e0, e1).start()
                if n == 3:
                    late_copy(p).start()
                die(place(p, n, k0, k1)).start()

    pass_on(1, (1, 2))
    pass_on(2, (2,))
    pass_on(3, (2,))
    pass_on(4, ())
    pass_on(5, ())
    pass_on(6, ())
    pass_on(7, ())
    sends = out.at[pl.ds(0, 7 * UNITS - sum(LATE_UNITS))]
    remote(sends, sends, is_, ir.at[0], partner).wait_send()
    half = out.at[pl.ds(0, 8 * UNITS - sum(LATE_UNITS))]
    die(half).wait_send()
    die(half).wait_recv()
    for p in range(3):
        late_copy(p).wait()


def step(lr, grad, w, m, v, mask):
    f32, bf16 = jnp.float32, jnp.bfloat16
    dma = pltpu.SemaphoreType.DMA
    flat = lambda a: pltpu.with_memory_space_constraint(a.reshape(ROWS, LANES), pltpu.HBM)
    hbm = pl.BlockSpec(memory_space=pl.ANY)
    vmem = pl.BlockSpec(memory_space=pltpu.VMEM)
    state = pltpu.VMEM((ROWS, LANES), f32)
    return pl.pallas_call(
        step_kernel,
        out_shape=(
            state, state, state, pltpu.VMEM((8, LANES), f32),
            pltpu.VMEM((NDEV * UNITS, 4, LANES), bf16),
            *[pltpu.HBM((n, 4, LANES), bf16) for n in LATE_UNITS],
            pltpu.HBM((96, 1, CW), bf16), pltpu.HBM((48, CR, LANES), f32), pltpu.HBM((24, CR, LANES), f32),
        ),
        in_specs=[hbm] * 6,
        out_specs=(vmem,) * 5 + (hbm,) * 6,
        scratch_shapes=[
            pltpu.VMEM((1, 1), f32),
            pltpu.VMEM((DEPTH, 1, CW), bf16),
            pltpu.VMEM((DEPTH, 1, CW), bf16),
            pltpu.VMEM((DEPTH, CR, LANES), f32),
            pltpu.VMEM((DEPTH, CR, LANES), f32),
            pltpu.VMEM((1, CW), bf16),
            pltpu.VMEM((3, 2, CR, LANES), bf16),
            pltpu.VMEM((3, 2, CR, LANES), bf16),
            pltpu.VMEM((ROWS, LANES), jnp.int32),
            pltpu.VMEM((4 * GROUPS, CR, LANES), f32),
            pltpu.VMEM((12, CR, LANES), f32),
            pltpu.VMEM((8, LANES), f32),
            pltpu.VMEM((NDEV, 8, LANES), f32),
            dma(()), dma(()),
            dma(()), dma((LATE + 2,)), dma((GROUPS,)),
            dma((4,)), dma((4,)), dma((12,)),
            dma(()), dma(()),
            dma((DEPTH,)), dma((DEPTH,)), dma((DEPTH,)), dma((DEPTH,)),
            dma((5,)), dma((3,)),
            dma(()), dma((3 * sum(len(e) - 1 for e in PIECES.values()),)), dma(()), dma(()),
        ],
        compiler_params=pltpu.CompilerParams(collective_id=0, has_side_effects=True, vmem_limit_bytes=22 * 1024 * 1024),
        name='step',
    )(lr.reshape(1, 1), grad, flat(w), flat(m), flat(v), flat(mask))


def publish_kernel(p_in, w_in, m_in, n_in, p_out, w_out, m_out, n_out, big, small):
    me = lax.axis_index('dp')
    base = me - me % 2
    late = late_blocks()
    spans = []
    for n in range(7):
        block = base
        for bit in range(3):
            if (n >> bit) & 1:
                block = block + step_of(me, bit)
        spans.append((block * UNITS, 2 * UNITS))
    for c in range(2):
        for p in range(3):
            spans.append(((late + c) * UNITS + end_of(p, 0), end_of(p, LATE_FROM) - end_of(p, 0)))
    copies = [pltpu.make_async_copy(p_in.at[pl.ds(a, n)], p_out.at[pl.ds(a, n)], big.at[i]) for i, (a, n) in enumerate(spans)]
    copies += [pltpu.make_async_copy(a, b, small.at[i]) for i, (a, b) in enumerate(((w_in, w_out), (m_in, m_out)))]
    for c in copies:
        c.start()
    n_out[...] = n_in[0, 0:1]
    for c in copies:
        c.wait()


def publish(arrays, norm):
    dma = pltpu.SemaphoreType.DMA
    vmem = pl.BlockSpec(memory_space=pltpu.VMEM)
    hbm = pl.BlockSpec(memory_space=pl.ANY)
    arrays = [pltpu.with_memory_space_constraint(a, pltpu.VMEM) for a in arrays]
    norm = pltpu.with_memory_space_constraint(norm, pltpu.VMEM)
    return pl.pallas_call(
        publish_kernel,
        out_shape=[jax.ShapeDtypeStruct(a.shape, a.dtype) for a in arrays] + [jax.ShapeDtypeStruct((1,), jnp.float32)],
        in_specs=[vmem] * 4,
        out_specs=[hbm] * 3 + [vmem],
        scratch_shapes=[dma((13,)), dma((2,))],
        compiler_params=pltpu.CompilerParams(vmem_limit_bytes=1024 * 1024),
        cost_estimate=pl.CostEstimate(flops=40_000_000, bytes_accessed=40_000_000, transcendentals=0),
        name='publish',
    )(*arrays, norm)


def late_blocks():
    me = lax.axis_index('dp')
    return me - me % 2 + step_of(me, 0) + step_of(me, 1) + step_of(me, 2)


def place_late(params, pieces, other, extra=()):
    def kernel(p_in, piece0, piece1, piece2, *refs):
        p_out, sem = refs[-2 - len(extra)], refs[-1]
        core = lax.axis_index('dp') % 2
        block = late_blocks() + (1 - core if other else core)
        copies = []
        for p, piece in enumerate((piece0, piece1, piece2)):
            here = p_out.at[pl.ds(block * UNITS + end_of(p, LATE_FROM), LATE_UNITS[p])]
            copies.append(pltpu.make_async_copy(piece, here, sem.at[p]))
        if extra:
            copies.append(pltpu.make_async_copy(refs[0], refs[2], sem.at[3]))
        for c in copies:
            c.start()
        for c in copies:
            c.wait()

    hbm = pl.BlockSpec(memory_space=pl.ANY)
    vmem = pl.BlockSpec(memory_space=pltpu.VMEM)
    return pl.pallas_call(
        kernel,
        out_shape=[jax.ShapeDtypeStruct(a.shape, a.dtype) for a in (params, *extra)],
        in_specs=[hbm] + [vmem] * (3 + len(extra)),
        out_specs=[hbm] * (1 + len(extra)),
        scratch_shapes=[pltpu.SemaphoreType.DMA((3 + len(extra),))],
        input_output_aliases={0: 0},
        compiler_params=pltpu.CompilerParams(vmem_limit_bytes=4 * 1024 * 1024),
        cost_estimate=pl.CostEstimate(flops=4_000_000, bytes_accessed=4_000_000, transcendentals=0),
        name='place_other' if other else 'place_own',
    )(params, *pieces, *[pltpu.with_memory_space_constraint(a, pltpu.VMEM) for a in extra])


def solution(mesh):
    def local_step(grad_row, master, mom_first, mom_second, decay_mask, learn_rate):
        w, m, v, norm, params, late0, late1, late2, *_ = step(learn_rate, grad_row, master, mom_first, mom_second, decay_mask)
        pieces = []
        for p, late in enumerate((late0, late1, late2)):
            stride = weight((p + 2) % 3)
            pieces.append(lax.ppermute(late, 'dp', [(d, d ^ stride) for d in range(NDEV)]))
        params, w, m, norm = publish([params, w, m], norm)
        *pieces, norm = lax.optimization_barrier((*pieces, norm))
        others = [lax.ppermute(piece, 'dp', [(d, d ^ 1) for d in range(NDEV)]) for piece in pieces]
        params, v = place_late(params, pieces, False, (v,))
        params, = place_late(params, others, True)
        return params.reshape(-1), w.reshape(-1), m.reshape(-1), v.reshape(-1), norm

    return jax.shard_map(local_step, mesh=mesh, in_specs=(P('dp', None), P('dp'), P('dp'), P('dp'), P('dp'), P()), out_specs=(P(), P('dp'), P('dp'), P('dp'), P()), check_vma=False)
```

```python
import jax
import jax.numpy as jnp
from jax import lax
from jax.experimental import pallas as pl
from jax.experimental.pallas import tpu as pltpu
from jax.sharding import PartitionSpec as P

BETA_FIRST = 0.9
BETA_SECOND = 0.95
ADAM_EPS = 1e-8
CLIP_EPS = 1e-6
WEIGHT_DECAY = 0.1
ADAM_STEP = 10

NDEV = 16
LANES = 128
ROWS = 6908
ROWS_PAD = 6912
CHUNKS = 12
CR = 576
CW = CR * LANES
SLAB = 144
NSLAB = CR // SLAB
DEPTH = 4
GROUPS = 6
UNITS = ROWS // 4
LATE = 12
PIECES = {1: (0, 4), 2: (0, 4), 3: (0, 4), 4: (0, 4), 5: (0, 3, 4), 6: (0, 3, 4), 7: (0, 0.625)}
LATE_FROM = 0.625
AG_UNITS = 144

MESH = pl.DeviceIdType.MESH


def weight(axis):
    return 2 + axis + axis * axis


def step_of(me, axis):
    w = weight(axis)
    return (1 - 2 * ((me // w) % 2)) * w


def chunk_row(q):
    return CR * q - 4 * (q // (CHUNKS - 1))


def end_of(p, k):
    return min(int(AG_UNITS * (4 * p + k)), UNITS)


LATE_UNITS = [end_of(p, 4) - end_of(p, LATE_FROM) for p in range(3)]


def remote(src, dst, ssem, rsem, dev):
    return pltpu.make_async_remote_copy(src_ref=src, dst_ref=dst, send_sem=ssem, recv_sem=rsem, device_id=(dev,), device_id_type=MESH)


def adam_slab(lr, clip, g, w, m, v, mask):
    h = g * clip
    m_new = BETA_FIRST * m + (1.0 - BETA_FIRST) * h
    v_new = BETA_SECOND * v + (1.0 - BETA_SECOND) * h * h
    step_dir = (m_new / (1.0 - BETA_FIRST ** ADAM_STEP)) / (jnp.sqrt(v_new / (1.0 - BETA_SECOND ** ADAM_STEP)) + ADAM_EPS)
    w_new = w - lr * (step_dir + WEIGHT_DECAY * mask.astype(jnp.float32) * w)
    return w_new, m_new, v_new


def step_kernel(lr_in, grad, w_in, m_in, v_in, mask_in, w, m, v, norm_out, out, late0, late1, late2, prow, r1, r2,
                lr, own, par, st1, st2, early, raw, first, mask, sb, r3, acc, nrm,
                fs, fr, psend, precv, sent, s1r, s2r, s3r, ns, nr, lo, lp, l1, l2, ld, is_, ir, ds_, dr):
    me = lax.axis_index('dp')
    partner = me + 1 - 2 * (me % 2)
    near = [me + step_of(me, a) for a in range(3)]

    base_of = {1: 0, 2: 48, 3: 72, 4: 84}
    count_of = {1: 48, 2: 24, 3: 12, 4: 12}

    def decode(phase, t):
        if phase == 1:
            if isinstance(t, int) and t < 12:
                return t % 3, 0, t // 3
            return (t // 4) % 3, t // 12, t % 4
        if phase == 2:
            return (t // 2) % 3, t // 6, t % 2
        return t % 3, t // 3, 0

    def where(phase, t):
        p, k, j = decode(phase, t)
        if phase == 1:
            o1, o2, o3 = 1, j % 2, j // 2
        elif phase == 2:
            o1, o2, o3 = 0, 1, j
        else:
            o1, o2, o3 = 0, 0, 1 if phase == 3 else 0
        shift = o1 * step_of(me, p) + o2 * step_of(me, (p + 1) % 3) + o3 * step_of(me, (p + 2) % 3)
        return shift, 4 * p + k

    def grad_slice(block, q):
        start = pl.multiple_of((block * ROWS + chunk_row(q)) * LANES, LANES)
        return grad.at[:, pl.ds(start, CW)]

    core = me % 2

    def first_load(p, c):
        shift, q = where(1, p)
        stage = par if c else own
        return pltpu.make_async_copy(grad_slice(me - core + c + shift, q), stage.at[p], (lp if c else lo).at[p])

    def first_copy(p, c):
        dev = me - core + c + step_of(me, p)
        return remote(raw.at[p, c], first.at[p, core], fs, fr, dev)

    def all_first(here):
        return remote(here, here, fs, fr, partner)

    def early_copy():
        shift, q = where(1, 3)
        return remote(grad_slice(partner + shift, q), early, psend, precv.at[LATE + 1], partner)

    def partner_copy(phase, t):
        shift, q = where(phase, t)
        group = t // 4 if phase == 1 else LATE
        return remote(grad_slice(partner + shift, q), prow.at[base_of[phase] + t], psend, precv.at[group], partner)

    def rows_here(first, count, group):
        rows = prow.at[pl.ds(first, count)]
        return remote(rows, rows, psend, precv.at[group], partner)

    def own_load(phase, t):
        shift, q = where(phase, t)
        slot = t % DEPTH
        return pltpu.make_async_copy(grad_slice(me + shift, q), own.at[slot], lo.at[slot])

    def slots(g, count):
        return sb.at[pl.ds(4 * (g % GROUPS), count)]

    def s1_one(p, j):
        return remote(sb.at[4 * p + j], r1.at[16 * p + j], sent.at[p], s1r.at[0], me + step_of(me, p))

    def s1_copy(p, k):
        g = 3 * k + p
        return remote(slots(g, 4), r1.at[pl.ds((4 * p + k) * 4, 4)], sent.at[g % GROUPS], s1r.at[k], me + step_of(me, p))

    def s2_copy(p, k):
        g = 3 * k + p
        return remote(slots(g, 2), r2.at[pl.ds((4 * p + k) * 2, 2)], sent.at[g % GROUPS], s2r.at[k], me + step_of(me, (p + 1) % 3))

    def s3_copy(p, k):
        g = 3 * k + p
        return remote(sb.at[4 * (g % GROUPS)], r3.at[g], sent.at[g % GROUPS], s3r.at[g], me + step_of(me, (p + 2) % 3))

    def arrived(buf, count, sem):
        here = buf.at[pl.ds(0, count)]
        remote(here, here, sent.at[0], sem, partner).wait_recv()

    def left(g, count):
        here = slots(g, count)
        remote(here, here, sent.at[g % GROUPS], s1r.at[0], partner).wait_send()

    def left_three(g):
        here = sb.at[pl.ds(4 * (g % GROUPS) + 1, 3)]
        remote(here, here, sent.at[g % GROUPS], s1r.at[0], partner).wait_send()

    def sources(phase, t):
        p, k, j = decode(phase, t)
        q = 4 * p + k
        if phase == 2:
            return 4 * q + 2 * j + 1, None
        if phase == 3:
            return 4 * q + 2, 2 * q + 1
        return 4 * q, 2 * q

    def loads(phase, t):
        slot = t % DEPTH
        copies = [own_load(phase, t), pltpu.make_async_copy(prow.at[base_of[phase] + t], par.at[slot], lp.at[slot])]
        if phase > 1:
            i1, i2 = sources(phase, t)
            if not (phase == 4 and isinstance(t, int) and t < 3):
                copies.append(pltpu.make_async_copy(r1.at[i1], st1.at[slot], l1.at[slot]))
            if phase > 2:
                copies.append(pltpu.make_async_copy(r2.at[i2], st2.at[slot], l2.at[slot]))
        return copies

    def when(cond, fn):
        if isinstance(cond, bool):
            if cond:
                fn()
        else:
            pl.when(cond)(fn)

    def start_loads(phase, t):
        p, k, j = decode(phase, t)
        if phase == 1:
            when(t % 4 == 0, lambda: rows_here(t, 4, t // 4).wait_recv())
        elif phase == 2:
            when(t == 0, lambda: arrived(r1, 9, s1r.at[0]))
            when((t % 6 == 0) & (t >= 6), lambda: arrived(r1, 12, s1r.at[k]))
        elif phase == 3:
            when(p == 0, lambda: arrived(r2, 6, s2r.at[k]))
        for c in loads(phase, t):
            c.start()

    def slab_cols(i):
        return pl.ds(pl.multiple_of(i * (SLAB * LANES), SLAB * LANES), SLAB * LANES)

    def chip_sum(slot, i, other=None):
        theirs = par[slot, :, slab_cols(i)] if other is None else other[:, slab_cols(i)]
        total = own[slot, :, slab_cols(i)].astype(jnp.float32) + theirs.astype(jnp.float32)
        return total.reshape(SLAB, LANES)

    def slabs(fn):
        def one(i, _):
            fn(i, pl.ds(pl.multiple_of(i * SLAB, SLAB), SLAB))
            return 0
        lax.fori_loop(0, NSLAB, one, 0)

    def loop(lo_t, hi_t, fn):
        def one(t, _):
            fn(t)
            return 0
        lax.fori_loop(lo_t, hi_t, one, 0)

    def run_phase(phase, body, first=0, static=0):
        n = count_of[phase]
        for t in range(first, first + DEPTH - 1):
            start_loads(phase, t)

        def one(t):
            when(t + DEPTH - 1 < n, lambda: start_loads(phase, t + DEPTH - 1))
            for c in loads(phase, t):
                c.wait()
            body(t)
        for t in range(first, static):
            one(t)
        loop(max(first, static), n, one)

    barrier = pltpu.get_barrier_semaphore()
    for other in [partner] + near + [n + partner - me for n in near]:
        pl.semaphore_signal(barrier, inc=1, device_id=(other,), device_id_type=MESH)
    for p in range(3):
        for c in range(2):
            first_load(p, c).start()
    own_load(1, 3).start()
    for p in range(3):
        for c in range(2):
            first_load(p, c).wait()
            stage = par if c else own

            def fn(i, rows):
                mine = stage[p, :, slab_cols(i)].astype(jnp.float32).reshape(SLAB, LANES)
                raw[p, c, rows, :] = mine.astype(jnp.bfloat16)
            slabs(fn)
            if p == 0 and c == 0:
                pl.semaphore_wait(barrier, 7)
            first_copy(p, c).start()
        if p == 0:
            early_copy().start()
    for u in range(4, 12):
        partner_copy(1, u).start()
    own_load(1, 3).wait()
    early_copy().wait_recv()

    def fn(i, rows):
        sb[1, rows, :] = chip_sum(3, i, early)
    slabs(fn)
    s1_one(0, 1).start()
    loop(12, 48, lambda t: partner_copy(1, t).start())

    def phase1(t):
        p, k, j = decode(1, t)
        g = 3 * k + p
        if not isinstance(t, int):
            when((t >= 24) & (t < 36) & (j == 0), lambda: left_three(g))
            when((t >= 36) & (j == 0), lambda: left(g, 4))
        slot = t % DEPTH

        def fn(i, rows):
            sb[4 * (g % GROUPS) + j, rows, :] = chip_sum(slot, i)
        slabs(fn)
        if isinstance(t, int):
            s1_one(p, j).start()
        else:
            when(j == 3, lambda: s1_copy(p, k).start())

    def phase2(t):
        p, k, j = decode(2, t)
        g = 3 * k + p
        when((j == 0) & (t < 12), lambda: left(g, 4))
        when((j == 0) & (t >= 12), lambda: left(g, 2))
        slot = t % DEPTH

        def fn(i, rows):
            sb[4 * (g % GROUPS) + j, rows, :] = chip_sum(slot, i) + st1[slot, rows, :]
        slabs(fn)
        when(j == 1, lambda: s2_copy(p, k).start())

    def phase3(t):
        p, k, _ = decode(3, t)
        when(t < 6, lambda: left(t, 2))
        when(t >= 6, lambda: left(t, 1))
        slot = t % DEPTH

        def fn(i, rows):
            sb[4 * (t % GROUPS), rows, :] = chip_sum(slot, i) + st1[slot, rows, :] + st2[slot, rows, :]
        slabs(fn)
        s3_copy(p, k).start()

    def early_sum(t):
        return 4 * (t // 3) + 1 + t % 3

    def phase4(t):
        slot = t % DEPTH

        def fn(i, rows):
            if isinstance(t, int):
                r1_part = first[t, 0, rows, :].astype(jnp.float32) + first[t, 1, rows, :].astype(jnp.float32)
            else:
                r1_part = st1[slot, rows, :]
            sb[early_sum(t), rows, :] = chip_sum(slot, i) + r1_part + st2[slot, rows, :]
        slabs(fn)

    run_phase(1, phase1, DEPTH, 12)
    for phase in (2, 3, 4):
        loop(0, count_of[phase], lambda t, phase=phase: partner_copy(phase, t).start())
    rows_here(48, 48, LATE).wait_recv()

    pairs = ((w_in, w), (m_in, m), (v_in, v), (mask_in, mask), (lr_in, lr))
    states = [pltpu.make_async_copy(a, b, ld.at[i]) for i, (a, b) in enumerate(pairs)]
    for c in states:
        c.start()
    run_phase(2, phase2)
    for c in states:
        c.wait()
    rows_here(4, 92, LATE).wait_send()
    early_copy().wait_send()
    all_first(raw).wait_send()
    all_first(first).wait_recv()
    run_phase(3, phase3)
    run_phase(4, phase4, 0, 3)

    acc[...] = jnp.zeros_like(acc)

    def finish(t, skip):
        s3_copy(t % 3, t // 3).wait_recv()

        def fn(i, rows):
            g = (sb[early_sum(t), rows, :] + r3[t, rows, :]) * (1.0 / NDEV)
            r3[t, rows, :] = g
            sq = g * g
            if skip:
                row = lax.broadcasted_iota(jnp.int32, (SLAB, LANES), 0) + i * SLAB
                sq = jnp.where(row < skip, 0.0, sq)
            acc[...] += jnp.sum(sq.reshape(SLAB // 8, 8, LANES), axis=0)
        slabs(fn)

    loop(0, 11, lambda t: finish(t, 0))
    finish(11, 4)

    nrm[me] = acc[...]

    def norm_copy(i):
        return remote(acc, nrm.at[me], ns, nr, i)

    others = nrm.at[pl.ds(0, NDEV - 1)]
    all_norms = remote(others, others, ns, nr, partner)
    far = sum(step_of(me, a) for a in range(3))
    hops = [step_of(me, a) for a in range(3)]
    for shift in [far] + [far - h for h in hops] + hops:
        for dev in (me + shift, partner + shift):
            norm_copy(dev).start()
    norm_copy(partner).start()
    for g in range(6, 12):
        left(g, 1)
    all_norms.wait_recv()
    total = nrm[0]
    for i in range(1, NDEV):
        total = total + nrm[i]
    norm = jnp.sqrt(jnp.sum(total, keepdims=True))
    norm_out[...] = jnp.broadcast_to(norm, norm_out.shape)
    clip = jnp.minimum(1.0, 1.0 / (norm + CLIP_EPS))
    rate = lr[...]

    def block_of(p, n):
        block = me
        for bit in range(3):
            if (n >> bit) & 1:
                block = block + step_of(me, (p + bit) % 3)
        return block

    def place(p, n, k0, k1):
        return out.at[pl.ds(block_of(p, n) * UNITS + end_of(p, k0), end_of(p, k1) - end_of(p, k0))]

    def late_copy(p):
        ref, n = (late0, late1, late2)[p], LATE_UNITS[p]
        start = block_of(p, 3) * UNITS + end_of(p, LATE_FROM)

        def some(i, _):
            ref[pl.ds(i * 36, 36)] = out[pl.ds(start + i * 36, 36)]
            return 0
        lax.fori_loop(0, n // 36, some, 0)
        done = n // 36 * 36
        if done < n:
            ref[done:n] = out[pl.ds(start + done, n - done)]

    def ir_index(p, n, k0):
        before = sum(len(PIECES[b]) - 1 for b in range(1, n))
        piece = sum(1 for edge in PIECES[n][1:] if edge <= k0)
        return 3 * (before + piece) + p

    def ici(p, n, hop, k0, k1):
        here = place(p, n, k0, k1)
        return remote(here, here, is_, ir.at[ir_index(p, n | (1 << hop), k0)], near[(p + hop) % 3])

    def arrival(p, n, k0, k1):
        here = place(p, n, k0, k1)
        return remote(here, here, is_, ir.at[ir_index(p, n, k0)], partner)

    def die(here):
        return remote(here, here, ds_, dr, partner)

    def update(p, k, lo_slab=0, hi_slab=NSLAB):
        t = 3 * k + p
        q = 4 * p + k
        short = q == CHUNKS - 1

        def slab(row0, n):
            rows = pl.ds(row0 + q * CR, n)
            src = pl.ds(row0 + 4, n) if short else pl.ds(row0, n)
            w_new, m_new, v_new = adam_slab(rate, clip, r3[t, src, :], w[rows, :], m[rows, :], v[rows, :], mask[rows, :])
            w[rows, :] = w_new
            m[rows, :] = m_new
            v[rows, :] = v_new
            return w_new.astype(jnp.bfloat16).reshape(n // 4, 4, LANES)

        base = me * UNITS + q * AG_UNITS
        if short:
            for i in range(0, CR, SLAB):
                n = min(SLAB, ROWS - q * CR - i)
                out[pl.ds(base + i // 4, n // 4)] = slab(i, n)
        else:
            def one(i, _):
                out[pl.ds(base + i * (SLAB // 4), SLAB // 4)] = slab(pl.multiple_of(i * SLAB, SLAB), SLAB)
                return 0
            lax.fori_loop(lo_slab, hi_slab, one, 0)

    for p in range(3):
        for k0, k1 in ((0, 0.25), (0.25, 1)) if p == 0 else ((0, 1),):
            update(p, 0, int(k0 * NSLAB), int(k1 * NSLAB))
            for hop in range(3):
                ici(p, 0, hop, k0, k1).start()
    for k in range(1, 4):
        for p in range(3):
            update(p, k)
            ici(p, 0, 0, k, k + 1).start()
    for hop in (1, 2):
        for p in range(3):
            ici(p, 0, hop, 1, 4).start()
    die(out.at[pl.ds(me * UNITS, UNITS)]).start()
    all_norms.wait_send()

    def pass_on(n, hops):
        for k0, k1 in zip(PIECES[n], PIECES[n][1:]):
            for p in range(3):
                arrival(p, n, k0, k1).wait_recv()
                for hop in hops:
                    last = min(k1, PIECES[n | (1 << hop)][-1])
                    edges = [k0] + [e for e in PIECES[n | (1 << hop)] if k0 < e < last] + [last]
                    for e0, e1 in zip(edges, edges[1:]):
                        ici(p, n, hop, e0, e1).start()
                if n == 3:
                    late_copy(p)
                die(place(p, n, k0, k1)).start()

    pass_on(1, (1, 2))
    pass_on(2, (2,))
    pass_on(3, (2,))
    pass_on(4, ())
    pass_on(5, ())
    pass_on(6, ())
    pass_on(7, ())
    sends = out.at[pl.ds(0, 7 * UNITS - sum(LATE_UNITS))]
    remote(sends, sends, is_, ir.at[0], partner).wait_send()
    half = out.at[pl.ds(0, 8 * UNITS - sum(LATE_UNITS))]
    die(half).wait_send()
    die(half).wait_recv()


def step(lr, grad, w, m, v, mask):
    f32, bf16 = jnp.float32, jnp.bfloat16
    dma = pltpu.SemaphoreType.DMA
    flat = lambda a: pltpu.with_memory_space_constraint(a.reshape(ROWS, LANES), pltpu.HBM)
    hbm = pl.BlockSpec(memory_space=pl.ANY)
    vmem = pl.BlockSpec(memory_space=pltpu.VMEM)
    state = pltpu.VMEM((ROWS, LANES), f32)
    return pl.pallas_call(
        step_kernel,
        out_shape=(
            state, state, state, pltpu.VMEM((8, LANES), f32),
            pltpu.VMEM((NDEV * UNITS, 4, LANES), bf16),
            *[pltpu.VMEM((n, 4, LANES), bf16) for n in LATE_UNITS],
            pltpu.HBM((96, 1, CW), bf16), pltpu.HBM((48, CR, LANES), f32), pltpu.HBM((24, CR, LANES), f32),
        ),
        in_specs=[hbm] * 6,
        out_specs=(vmem,) * 8 + (hbm,) * 3,
        scratch_shapes=[
            pltpu.VMEM((1, 1), f32),
            pltpu.VMEM((DEPTH, 1, CW), bf16),
            pltpu.VMEM((DEPTH, 1, CW), bf16),
            pltpu.VMEM((DEPTH, CR, LANES), f32),
            pltpu.VMEM((DEPTH, CR, LANES), f32),
            pltpu.VMEM((1, CW), bf16),
            pltpu.VMEM((3, 2, CR, LANES), bf16),
            pltpu.VMEM((3, 2, CR, LANES), bf16),
            pltpu.VMEM((ROWS, LANES), jnp.int32),
            pltpu.VMEM((4 * GROUPS, CR, LANES), f32),
            pltpu.VMEM((12, CR, LANES), f32),
            pltpu.VMEM((8, LANES), f32),
            pltpu.VMEM((NDEV, 8, LANES), f32),
            dma(()), dma(()),
            dma(()), dma((LATE + 2,)), dma((GROUPS,)),
            dma((4,)), dma((4,)), dma((12,)),
            dma(()), dma(()),
            dma((DEPTH,)), dma((DEPTH,)), dma((DEPTH,)), dma((DEPTH,)),
            dma((5,)),
            dma(()), dma((3 * sum(len(e) - 1 for e in PIECES.values()),)), dma(()), dma(()),
        ],
        compiler_params=pltpu.CompilerParams(collective_id=0, has_side_effects=True, vmem_limit_bytes=22 * 1024 * 1024),
        name='step',
    )(lr.reshape(1, 1), grad, flat(w), flat(m), flat(v), flat(mask))


def publish_kernel(p_in, w_in, m_in, n_in, p_out, w_out, m_out, n_out, big, small):
    me = lax.axis_index('dp')
    base = me - me % 2
    late = late_blocks()
    spans = []
    for n in range(7):
        block = base
        for bit in range(3):
            if (n >> bit) & 1:
                block = block + step_of(me, bit)
        spans.append((block * UNITS, 2 * UNITS))
    for c in range(2):
        for p in range(3):
            spans.append(((late + c) * UNITS + end_of(p, 0), end_of(p, LATE_FROM) - end_of(p, 0)))
    copies = [pltpu.make_async_copy(p_in.at[pl.ds(a, n)], p_out.at[pl.ds(a, n)], big.at[i]) for i, (a, n) in enumerate(spans)]
    copies += [pltpu.make_async_copy(a, b, small.at[i]) for i, (a, b) in enumerate(((w_in, w_out), (m_in, m_out)))]
    for c in copies:
        c.start()
    n_out[...] = n_in[0, 0:1]
    for c in copies:
        c.wait()


def publish(arrays, norm):
    dma = pltpu.SemaphoreType.DMA
    vmem = pl.BlockSpec(memory_space=pltpu.VMEM)
    hbm = pl.BlockSpec(memory_space=pl.ANY)
    arrays = [pltpu.with_memory_space_constraint(a, pltpu.VMEM) for a in arrays]
    norm = pltpu.with_memory_space_constraint(norm, pltpu.VMEM)
    return pl.pallas_call(
        publish_kernel,
        out_shape=[jax.ShapeDtypeStruct(a.shape, a.dtype) for a in arrays] + [jax.ShapeDtypeStruct((1,), jnp.float32)],
        in_specs=[vmem] * 4,
        out_specs=[hbm] * 3 + [vmem],
        scratch_shapes=[dma((13,)), dma((2,))],
        compiler_params=pltpu.CompilerParams(vmem_limit_bytes=1024 * 1024),
        cost_estimate=pl.CostEstimate(flops=40_000_000, bytes_accessed=40_000_000, transcendentals=0),
        name='publish',
    )(*arrays, norm)


def late_blocks():
    me = lax.axis_index('dp')
    return me - me % 2 + step_of(me, 0) + step_of(me, 1) + step_of(me, 2)


def place_late(params, pieces, other, extra=()):
    def kernel(p_in, piece0, piece1, piece2, *refs):
        p_out, sem = refs[-2 - len(extra)], refs[-1]
        core = lax.axis_index('dp') % 2
        block = late_blocks() + (1 - core if other else core)
        copies = []
        for p, piece in enumerate((piece0, piece1, piece2)):
            here = p_out.at[pl.ds(block * UNITS + end_of(p, LATE_FROM), LATE_UNITS[p])]
            copies.append(pltpu.make_async_copy(piece, here, sem.at[p]))
        if extra:
            copies.append(pltpu.make_async_copy(refs[0], refs[2], sem.at[3]))
        for c in copies:
            c.start()
        for c in copies:
            c.wait()

    hbm = pl.BlockSpec(memory_space=pl.ANY)
    vmem = pl.BlockSpec(memory_space=pltpu.VMEM)
    return pl.pallas_call(
        kernel,
        out_shape=[jax.ShapeDtypeStruct(a.shape, a.dtype) for a in (params, *extra)],
        in_specs=[hbm] + [vmem] * (3 + len(extra)),
        out_specs=[hbm] * (1 + len(extra)),
        scratch_shapes=[pltpu.SemaphoreType.DMA((3 + len(extra),))],
        input_output_aliases={0: 0},
        compiler_params=pltpu.CompilerParams(vmem_limit_bytes=4 * 1024 * 1024),
        cost_estimate=pl.CostEstimate(flops=4_000_000, bytes_accessed=4_000_000, transcendentals=0),
        name='place_other' if other else 'place_own',
    )(params, *pieces, *[pltpu.with_memory_space_constraint(a, pltpu.VMEM) for a in extra])


def solution(mesh):
    def local_step(grad_row, master, mom_first, mom_second, decay_mask, learn_rate):
        w, m, v, norm, params, late0, late1, late2, *_ = step(learn_rate, grad_row, master, mom_first, mom_second, decay_mask)
        pieces = []
        for p, late in enumerate((late0, late1, late2)):
            stride = weight((p + 2) % 3)
            pieces.append(lax.ppermute(late, 'dp', [(d, d ^ stride) for d in range(NDEV)]))
        params, w, m, norm = publish([params, w, m], norm)
        *pieces, norm = lax.optimization_barrier((*pieces, norm))
        others = [lax.ppermute(piece, 'dp', [(d, d ^ 1) for d in range(NDEV)]) for piece in pieces]
        params, v = place_late(params, pieces, False, (v,))
        params, = place_late(params, others, True)
        return params.reshape(-1), w.reshape(-1), m.reshape(-1), v.reshape(-1), norm

    return jax.shard_map(local_step, mesh=mesh, in_specs=(P('dp', None), P('dp'), P('dp'), P('dp'), P('dp'), P()), out_specs=(P(), P('dp'), P('dp'), P('dp'), P()), check_vma=False)
```

```python
import jax
import jax.numpy as jnp
from jax import lax
from jax.experimental import pallas as pl
from jax.experimental.pallas import tpu as pltpu
from jax.sharding import PartitionSpec as P

BETA_FIRST = 0.9
BETA_SECOND = 0.95
ADAM_EPS = 1e-8
CLIP_EPS = 1e-6
WEIGHT_DECAY = 0.1
ADAM_STEP = 10

NDEV = 16
LANES = 128
ROWS = 6908
ROWS_PAD = 6912
CHUNKS = 12
CR = 576
CW = CR * LANES
SLAB = 144
NSLAB = CR // SLAB
DEPTH = 4
GROUPS = 6
UNITS = ROWS // 4
LATE = 12
PIECES = {1: (0, 4), 2: (0, 4), 3: (0, 4), 4: (0, 4), 5: (0, 3, 4), 6: (0, 2, 3, 4), 7: (0, 0.625)}
LATE_FROM = 0.625
AG_UNITS = 144

MESH = pl.DeviceIdType.MESH


def weight(axis):
    return 2 + axis + axis * axis


def step_of(me, axis):
    w = weight(axis)
    return (1 - 2 * ((me // w) % 2)) * w


def chunk_row(q):
    return CR * q - 4 * (q // (CHUNKS - 1))


def end_of(p, k):
    return min(int(AG_UNITS * (4 * p + k)), UNITS)


LATE_UNITS = [end_of(p, 4) - end_of(p, LATE_FROM) for p in range(3)]


def remote(src, dst, ssem, rsem, dev):
    return pltpu.make_async_remote_copy(src_ref=src, dst_ref=dst, send_sem=ssem, recv_sem=rsem, device_id=(dev,), device_id_type=MESH)


def adam_slab(lr, clip, g, w, m, v, mask):
    h = g * clip
    m_new = BETA_FIRST * m + (1.0 - BETA_FIRST) * h
    v_new = BETA_SECOND * v + (1.0 - BETA_SECOND) * h * h
    step_dir = (m_new / (1.0 - BETA_FIRST ** ADAM_STEP)) / (jnp.sqrt(v_new / (1.0 - BETA_SECOND ** ADAM_STEP)) + ADAM_EPS)
    w_new = w - lr * (step_dir + WEIGHT_DECAY * mask.astype(jnp.float32) * w)
    return w_new, m_new, v_new


def step_kernel(lr_in, grad, w_in, m_in, v_in, mask_in, w, m, v, norm_out, out, late0, late1, late2, prow, r1, r2,
                lr, own, par, st1, st2, early, raw, first, mask, sb, r3, acc, nrm,
                fs, fr, psend, precv, sent, s1r, s2r, s3r, ns, nr, lo, lp, l1, l2, ld, is_, ir, ds_, dr):
    me = lax.axis_index('dp')
    partner = me + 1 - 2 * (me % 2)
    near = [me + step_of(me, a) for a in range(3)]

    base_of = {1: 0, 2: 48, 3: 72, 4: 84}
    count_of = {1: 48, 2: 24, 3: 12, 4: 12}

    def decode(phase, t):
        if phase == 1:
            if isinstance(t, int) and t < 12:
                return t % 3, 0, t // 3
            return (t // 4) % 3, t // 12, t % 4
        if phase == 2:
            return (t // 2) % 3, t // 6, t % 2
        return t % 3, t // 3, 0

    def where(phase, t):
        p, k, j = decode(phase, t)
        if phase == 1:
            o1, o2, o3 = 1, j % 2, j // 2
        elif phase == 2:
            o1, o2, o3 = 0, 1, j
        else:
            o1, o2, o3 = 0, 0, 1 if phase == 3 else 0
        shift = o1 * step_of(me, p) + o2 * step_of(me, (p + 1) % 3) + o3 * step_of(me, (p + 2) % 3)
        return shift, 4 * p + k

    def grad_slice(block, q):
        start = pl.multiple_of((block * ROWS + chunk_row(q)) * LANES, LANES)
        return grad.at[:, pl.ds(start, CW)]

    core = me % 2

    def first_load(p, c):
        shift, q = where(1, p)
        stage = par if c else own
        return pltpu.make_async_copy(grad_slice(me - core + c + shift, q), stage.at[p], (lp if c else lo).at[p])

    def first_copy(p, c):
        dev = me - core + c + step_of(me, p)
        return remote(raw.at[p, c], first.at[p, core], fs, fr, dev)

    def all_first(here):
        return remote(here, here, fs, fr, partner)

    def early_copy():
        shift, q = where(1, 3)
        return remote(grad_slice(partner + shift, q), early, psend, precv.at[LATE + 1], partner)

    def partner_copy(phase, t):
        shift, q = where(phase, t)
        group = t // 4 if phase == 1 else LATE
        return remote(grad_slice(partner + shift, q), prow.at[base_of[phase] + t], psend, precv.at[group], partner)

    def rows_here(first, count, group):
        rows = prow.at[pl.ds(first, count)]
        return remote(rows, rows, psend, precv.at[group], partner)

    def own_load(phase, t):
        shift, q = where(phase, t)
        slot = t % DEPTH
        return pltpu.make_async_copy(grad_slice(me + shift, q), own.at[slot], lo.at[slot])

    def slots(g, count):
        return sb.at[pl.ds(4 * (g % GROUPS), count)]

    def s1_one(p, j):
        return remote(sb.at[4 * p + j], r1.at[16 * p + j], sent.at[p], s1r.at[0], me + step_of(me, p))

    def s1_copy(p, k):
        g = 3 * k + p
        return remote(slots(g, 4), r1.at[pl.ds((4 * p + k) * 4, 4)], sent.at[g % GROUPS], s1r.at[k], me + step_of(me, p))

    def s2_copy(p, k):
        g = 3 * k + p
        return remote(slots(g, 2), r2.at[pl.ds((4 * p + k) * 2, 2)], sent.at[g % GROUPS], s2r.at[k], me + step_of(me, (p + 1) % 3))

    def s3_copy(p, k):
        g = 3 * k + p
        return remote(sb.at[4 * (g % GROUPS)], r3.at[g], sent.at[g % GROUPS], s3r.at[g], me + step_of(me, (p + 2) % 3))

    def arrived(buf, count, sem):
        here = buf.at[pl.ds(0, count)]
        remote(here, here, sent.at[0], sem, partner).wait_recv()

    def left(g, count):
        here = slots(g, count)
        remote(here, here, sent.at[g % GROUPS], s1r.at[0], partner).wait_send()

    def left_three(g):
        here = sb.at[pl.ds(4 * (g % GROUPS) + 1, 3)]
        remote(here, here, sent.at[g % GROUPS], s1r.at[0], partner).wait_send()

    def sources(phase, t):
        p, k, j = decode(phase, t)
        q = 4 * p + k
        if phase == 2:
            return 4 * q + 2 * j + 1, None
        if phase == 3:
            return 4 * q + 2, 2 * q + 1
        return 4 * q, 2 * q

    def loads(phase, t):
        slot = t % DEPTH
        copies = [own_load(phase, t), pltpu.make_async_copy(prow.at[base_of[phase] + t], par.at[slot], lp.at[slot])]
        if phase > 1:
            i1, i2 = sources(phase, t)
            if not (phase == 4 and isinstance(t, int) and t < 3):
                copies.append(pltpu.make_async_copy(r1.at[i1], st1.at[slot], l1.at[slot]))
            if phase > 2:
                copies.append(pltpu.make_async_copy(r2.at[i2], st2.at[slot], l2.at[slot]))
        return copies

    def when(cond, fn):
        if isinstance(cond, bool):
            if cond:
                fn()
        else:
            pl.when(cond)(fn)

    def start_loads(phase, t):
        p, k, j = decode(phase, t)
        if phase == 1:
            when(t % 4 == 0, lambda: rows_here(t, 4, t // 4).wait_recv())
        elif phase == 2:
            when(t == 0, lambda: arrived(r1, 9, s1r.at[0]))
            when((t % 6 == 0) & (t >= 6), lambda: arrived(r1, 12, s1r.at[k]))
        elif phase == 3:
            when(p == 0, lambda: arrived(r2, 6, s2r.at[k]))
        for c in loads(phase, t):
            c.start()

    def slab_cols(i):
        return pl.ds(pl.multiple_of(i * (SLAB * LANES), SLAB * LANES), SLAB * LANES)

    def chip_sum(slot, i, other=None):
        theirs = par[slot, :, slab_cols(i)] if other is None else other[:, slab_cols(i)]
        total = own[slot, :, slab_cols(i)].astype(jnp.float32) + theirs.astype(jnp.float32)
        return total.reshape(SLAB, LANES)

    def slabs(fn):
        def one(i, _):
            fn(i, pl.ds(pl.multiple_of(i * SLAB, SLAB), SLAB))
            return 0
        lax.fori_loop(0, NSLAB, one, 0)

    def loop(lo_t, hi_t, fn):
        def one(t, _):
            fn(t)
            return 0
        lax.fori_loop(lo_t, hi_t, one, 0)

    def run_phase(phase, body, first=0, static=0):
        n = count_of[phase]
        for t in range(first, first + DEPTH - 1):
            start_loads(phase, t)

        def one(t):
            when(t + DEPTH - 1 < n, lambda: start_loads(phase, t + DEPTH - 1))
            for c in loads(phase, t):
                c.wait()
            body(t)
        for t in range(first, static):
            one(t)
        loop(max(first, static), n, one)

    barrier = pltpu.get_barrier_semaphore()
    for other in [partner] + near + [n + partner - me for n in near]:
        pl.semaphore_signal(barrier, inc=1, device_id=(other,), device_id_type=MESH)
    for p in range(3):
        for c in range(2):
            first_load(p, c).start()
    own_load(1, 3).start()
    for p in range(3):
        for c in range(2):
            first_load(p, c).wait()
            stage = par if c else own

            def fn(i, rows):
                mine = stage[p, :, slab_cols(i)].astype(jnp.float32).reshape(SLAB, LANES)
                raw[p, c, rows, :] = mine.astype(jnp.bfloat16)
            slabs(fn)
            if p == 0 and c == 0:
                pl.semaphore_wait(barrier, 7)
            first_copy(p, c).start()
        if p == 0:
            early_copy().start()
    for u in range(4, 12):
        partner_copy(1, u).start()
    own_load(1, 3).wait()
    early_copy().wait_recv()

    def fn(i, rows):
        sb[1, rows, :] = chip_sum(3, i, early)
    slabs(fn)
    s1_one(0, 1).start()
    loop(12, 48, lambda t: partner_copy(1, t).start())

    def phase1(t):
        p, k, j = decode(1, t)
        g = 3 * k + p
        if not isinstance(t, int):
            when((t >= 24) & (t < 36) & (j == 0), lambda: left_three(g))
            when((t >= 36) & (j == 0), lambda: left(g, 4))
        slot = t % DEPTH

        def fn(i, rows):
            sb[4 * (g % GROUPS) + j, rows, :] = chip_sum(slot, i)
        slabs(fn)
        if isinstance(t, int):
            s1_one(p, j).start()
        else:
            when(j == 3, lambda: s1_copy(p, k).start())

    def phase2(t):
        p, k, j = decode(2, t)
        g = 3 * k + p
        when((j == 0) & (t < 12), lambda: left(g, 4))
        when((j == 0) & (t >= 12), lambda: left(g, 2))
        slot = t % DEPTH

        def fn(i, rows):
            sb[4 * (g % GROUPS) + j, rows, :] = chip_sum(slot, i) + st1[slot, rows, :]
        slabs(fn)
        when(j == 1, lambda: s2_copy(p, k).start())

    def phase3(t):
        p, k, _ = decode(3, t)
        when(t < 6, lambda: left(t, 2))
        when(t >= 6, lambda: left(t, 1))
        slot = t % DEPTH

        def fn(i, rows):
            sb[4 * (t % GROUPS), rows, :] = chip_sum(slot, i) + st1[slot, rows, :] + st2[slot, rows, :]
        slabs(fn)
        s3_copy(p, k).start()

    def early_sum(t):
        return 4 * (t // 3) + 1 + t % 3

    def phase4(t):
        slot = t % DEPTH

        def fn(i, rows):
            if isinstance(t, int):
                r1_part = first[t, 0, rows, :].astype(jnp.float32) + first[t, 1, rows, :].astype(jnp.float32)
            else:
                r1_part = st1[slot, rows, :]
            sb[early_sum(t), rows, :] = chip_sum(slot, i) + r1_part + st2[slot, rows, :]
        slabs(fn)

    run_phase(1, phase1, DEPTH, 12)
    for phase in (2, 3, 4):
        loop(0, count_of[phase], lambda t, phase=phase: partner_copy(phase, t).start())
    rows_here(48, 48, LATE).wait_recv()

    pairs = ((w_in, w), (m_in, m), (v_in, v), (mask_in, mask), (lr_in, lr))
    states = [pltpu.make_async_copy(a, b, ld.at[i]) for i, (a, b) in enumerate(pairs)]
    for c in states:
        c.start()
    run_phase(2, phase2)
    for c in states:
        c.wait()
    rows_here(4, 92, LATE).wait_send()
    early_copy().wait_send()
    all_first(raw).wait_send()
    all_first(first).wait_recv()
    run_phase(3, phase3)
    run_phase(4, phase4, 0, 3)

    acc[...] = jnp.zeros_like(acc)

    def finish(t, skip):
        s3_copy(t % 3, t // 3).wait_recv()

        def fn(i, rows):
            g = (sb[early_sum(t), rows, :] + r3[t, rows, :]) * (1.0 / NDEV)
            r3[t, rows, :] = g
            sq = g * g
            if skip:
                row = lax.broadcasted_iota(jnp.int32, (SLAB, LANES), 0) + i * SLAB
                sq = jnp.where(row < skip, 0.0, sq)
            acc[...] += jnp.sum(sq.reshape(SLAB // 8, 8, LANES), axis=0)
        slabs(fn)

    loop(0, 11, lambda t: finish(t, 0))
    finish(11, 4)

    nrm[me] = acc[...]

    def norm_copy(i):
        return remote(acc, nrm.at[me], ns, nr, i)

    others = nrm.at[pl.ds(0, NDEV - 1)]
    all_norms = remote(others, others, ns, nr, partner)
    far = sum(step_of(me, a) for a in range(3))
    hops = [step_of(me, a) for a in range(3)]
    for shift in [far] + [far - h for h in hops] + hops:
        for dev in (me + shift, partner + shift):
            norm_copy(dev).start()
    norm_copy(partner).start()
    for g in range(6, 12):
        left(g, 1)
    all_norms.wait_recv()
    total = nrm[0]
    for i in range(1, NDEV):
        total = total + nrm[i]
    norm = jnp.sqrt(jnp.sum(total, keepdims=True))
    norm_out[...] = jnp.broadcast_to(norm, norm_out.shape)
    clip = jnp.minimum(1.0, 1.0 / (norm + CLIP_EPS))
    rate = lr[...]

    def block_of(p, n):
        block = me
        for bit in range(3):
            if (n >> bit) & 1:
                block = block + step_of(me, (p + bit) % 3)
        return block

    def place(p, n, k0, k1):
        return out.at[pl.ds(block_of(p, n) * UNITS + end_of(p, k0), end_of(p, k1) - end_of(p, k0))]

    def late_copy(p):
        ref, n = (late0, late1, late2)[p], LATE_UNITS[p]
        start = block_of(p, 3) * UNITS + end_of(p, LATE_FROM)

        def some(i, _):
            ref[pl.ds(i * 36, 36)] = out[pl.ds(start + i * 36, 36)]
            return 0
        lax.fori_loop(0, n // 36, some, 0)
        done = n // 36 * 36
        if done < n:
            ref[done:n] = out[pl.ds(start + done, n - done)]

    def ir_index(p, n, k0):
        before = sum(len(PIECES[b]) - 1 for b in range(1, n))
        piece = sum(1 for edge in PIECES[n][1:] if edge <= k0)
        return 3 * (before + piece) + p

    def ici(p, n, hop, k0, k1):
        here = place(p, n, k0, k1)
        return remote(here, here, is_, ir.at[ir_index(p, n | (1 << hop), k0)], near[(p + hop) % 3])

    def arrival(p, n, k0, k1):
        here = place(p, n, k0, k1)
        return remote(here, here, is_, ir.at[ir_index(p, n, k0)], partner)

    def die(here):
        return remote(here, here, ds_, dr, partner)

    def update(p, k, lo_slab=0, hi_slab=NSLAB):
        t = 3 * k + p
        q = 4 * p + k
        short = q == CHUNKS - 1

        def slab(row0, n):
            rows = pl.ds(row0 + q * CR, n)
            src = pl.ds(row0 + 4, n) if short else pl.ds(row0, n)
            w_new, m_new, v_new = adam_slab(rate, clip, r3[t, src, :], w[rows, :], m[rows, :], v[rows, :], mask[rows, :])
            w[rows, :] = w_new
            m[rows, :] = m_new
            v[rows, :] = v_new
            return w_new.astype(jnp.bfloat16).reshape(n // 4, 4, LANES)

        base = me * UNITS + q * AG_UNITS
        if short:
            for i in range(0, CR, SLAB):
                n = min(SLAB, ROWS - q * CR - i)
                out[pl.ds(base + i // 4, n // 4)] = slab(i, n)
        else:
            def one(i, _):
                out[pl.ds(base + i * (SLAB // 4), SLAB // 4)] = slab(pl.multiple_of(i * SLAB, SLAB), SLAB)
                return 0
            lax.fori_loop(lo_slab, hi_slab, one, 0)

    for p in range(3):
        for k0, k1 in ((0, 0.25), (0.25, 1)) if p == 0 else ((0, 1),):
            update(p, 0, int(k0 * NSLAB), int(k1 * NSLAB))
            for hop in range(3):
                ici(p, 0, hop, k0, k1).start()
    for k in range(1, 4):
        for p in range(3):
            update(p, k)
            ici(p, 0, 0, k, k + 1).start()
    for hop in (1, 2):
        for p in range(3):
            ici(p, 0, hop, 1, 4).start()
    die(out.at[pl.ds(me * UNITS, UNITS)]).start()
    all_norms.wait_send()

    def pass_on(n, hops):
        for k0, k1 in zip(PIECES[n], PIECES[n][1:]):
            for p in range(3):
                arrival(p, n, k0, k1).wait_recv()
                for hop in hops:
                    last = min(k1, PIECES[n | (1 << hop)][-1])
                    edges = [k0] + [e for e in PIECES[n | (1 << hop)] if k0 < e < last] + [last]
                    for e0, e1 in zip(edges, edges[1:]):
                        ici(p, n, hop, e0, e1).start()
                if n == 3:
                    late_copy(p)
                die(place(p, n, k0, k1)).start()

    pass_on(1, (1, 2))
    pass_on(2, (2,))
    pass_on(3, (2,))
    pass_on(4, ())
    pass_on(5, ())
    pass_on(6, ())
    pass_on(7, ())
    sends = out.at[pl.ds(0, 7 * UNITS - sum(LATE_UNITS))]
    remote(sends, sends, is_, ir.at[0], partner).wait_send()
    half = out.at[pl.ds(0, 8 * UNITS - sum(LATE_UNITS))]
    die(half).wait_send()
    die(half).wait_recv()


def step(lr, grad, w, m, v, mask):
    f32, bf16 = jnp.float32, jnp.bfloat16
    dma = pltpu.SemaphoreType.DMA
    flat = lambda a: pltpu.with_memory_space_constraint(a.reshape(ROWS, LANES), pltpu.HBM)
    hbm = pl.BlockSpec(memory_space=pl.ANY)
    vmem = pl.BlockSpec(memory_space=pltpu.VMEM)
    state = pltpu.VMEM((ROWS, LANES), f32)
    return pl.pallas_call(
        step_kernel,
        out_shape=(
            state, state, state, pltpu.VMEM((8, LANES), f32),
            pltpu.VMEM((NDEV * UNITS, 4, LANES), bf16),
            *[pltpu.VMEM((n, 4, LANES), bf16) for n in LATE_UNITS],
            pltpu.HBM((96, 1, CW), bf16), pltpu.HBM((48, CR, LANES), f32), pltpu.HBM((24, CR, LANES), f32),
        ),
        in_specs=[hbm] * 6,
        out_specs=(vmem,) * 8 + (hbm,) * 3,
        scratch_shapes=[
            pltpu.VMEM((1, 1), f32),
            pltpu.VMEM((DEPTH, 1, CW), bf16),
            pltpu.VMEM((DEPTH, 1, CW), bf16),
            pltpu.VMEM((DEPTH, CR, LANES), f32),
            pltpu.VMEM((DEPTH, CR, LANES), f32),
            pltpu.VMEM((1, CW), bf16),
            pltpu.VMEM((3, 2, CR, LANES), bf16),
            pltpu.VMEM((3, 2, CR, LANES), bf16),
            pltpu.VMEM((ROWS, LANES), jnp.int32),
            pltpu.VMEM((4 * GROUPS, CR, LANES), f32),
            pltpu.VMEM((12, CR, LANES), f32),
            pltpu.VMEM((8, LANES), f32),
            pltpu.VMEM((NDEV, 8, LANES), f32),
            dma(()), dma(()),
            dma(()), dma((LATE + 2,)), dma((GROUPS,)),
            dma((4,)), dma((4,)), dma((12,)),
            dma(()), dma(()),
            dma((DEPTH,)), dma((DEPTH,)), dma((DEPTH,)), dma((DEPTH,)),
            dma((5,)),
            dma(()), dma((3 * sum(len(e) - 1 for e in PIECES.values()),)), dma(()), dma(()),
        ],
        compiler_params=pltpu.CompilerParams(collective_id=0, has_side_effects=True, vmem_limit_bytes=22 * 1024 * 1024),
        name='step',
    )(lr.reshape(1, 1), grad, flat(w), flat(m), flat(v), flat(mask))


def publish_kernel(p_in, w_in, m_in, n_in, p_out, w_out, m_out, n_out, big, small):
    me = lax.axis_index('dp')
    base = me - me % 2
    late = late_blocks()
    spans = []
    for n in range(7):
        block = base
        for bit in range(3):
            if (n >> bit) & 1:
                block = block + step_of(me, bit)
        spans.append((block * UNITS, 2 * UNITS))
    for c in range(2):
        for p in range(3):
            spans.append(((late + c) * UNITS + end_of(p, 0), end_of(p, LATE_FROM) - end_of(p, 0)))
    copies = [pltpu.make_async_copy(p_in.at[pl.ds(a, n)], p_out.at[pl.ds(a, n)], big.at[i]) for i, (a, n) in enumerate(spans)]
    copies += [pltpu.make_async_copy(a, b, small.at[i]) for i, (a, b) in enumerate(((w_in, w_out), (m_in, m_out)))]
    for c in copies:
        c.start()
    n_out[...] = n_in[0, 0:1]
    for c in copies:
        c.wait()


def publish(arrays, norm):
    dma = pltpu.SemaphoreType.DMA
    vmem = pl.BlockSpec(memory_space=pltpu.VMEM)
    hbm = pl.BlockSpec(memory_space=pl.ANY)
    arrays = [pltpu.with_memory_space_constraint(a, pltpu.VMEM) for a in arrays]
    norm = pltpu.with_memory_space_constraint(norm, pltpu.VMEM)
    return pl.pallas_call(
        publish_kernel,
        out_shape=[jax.ShapeDtypeStruct(a.shape, a.dtype) for a in arrays] + [jax.ShapeDtypeStruct((1,), jnp.float32)],
        in_specs=[vmem] * 4,
        out_specs=[hbm] * 3 + [vmem],
        scratch_shapes=[dma((13,)), dma((2,))],
        compiler_params=pltpu.CompilerParams(vmem_limit_bytes=1024 * 1024),
        cost_estimate=pl.CostEstimate(flops=40_000_000, bytes_accessed=40_000_000, transcendentals=0),
        name='publish',
    )(*arrays, norm)


def late_blocks():
    me = lax.axis_index('dp')
    return me - me % 2 + step_of(me, 0) + step_of(me, 1) + step_of(me, 2)


def place_late(params, pieces, other, extra=()):
    def kernel(p_in, piece0, piece1, piece2, *refs):
        p_out, sem = refs[-2 - len(extra)], refs[-1]
        core = lax.axis_index('dp') % 2
        block = late_blocks() + (1 - core if other else core)
        copies = []
        for p, piece in enumerate((piece0, piece1, piece2)):
            here = p_out.at[pl.ds(block * UNITS + end_of(p, LATE_FROM), LATE_UNITS[p])]
            copies.append(pltpu.make_async_copy(piece, here, sem.at[p]))
        if extra:
            copies.append(pltpu.make_async_copy(refs[0], refs[2], sem.at[3]))
        for c in copies:
            c.start()
        for c in copies:
            c.wait()

    hbm = pl.BlockSpec(memory_space=pl.ANY)
    vmem = pl.BlockSpec(memory_space=pltpu.VMEM)
    return pl.pallas_call(
        kernel,
        out_shape=[jax.ShapeDtypeStruct(a.shape, a.dtype) for a in (params, *extra)],
        in_specs=[hbm] + [vmem] * (3 + len(extra)),
        out_specs=[hbm] * (1 + len(extra)),
        scratch_shapes=[pltpu.SemaphoreType.DMA((3 + len(extra),))],
        input_output_aliases={0: 0},
        compiler_params=pltpu.CompilerParams(vmem_limit_bytes=4 * 1024 * 1024),
        cost_estimate=pl.CostEstimate(flops=4_000_000, bytes_accessed=4_000_000, transcendentals=0),
        name='place_other' if other else 'place_own',
    )(params, *pieces, *[pltpu.with_memory_space_constraint(a, pltpu.VMEM) for a in extra])


def solution(mesh):
    def local_step(grad_row, master, mom_first, mom_second, decay_mask, learn_rate):
        w, m, v, norm, params, late0, late1, late2, *_ = step(learn_rate, grad_row, master, mom_first, mom_second, decay_mask)
        pieces = []
        for p, late in enumerate((late0, late1, late2)):
            stride = weight((p + 2) % 3)
            pieces.append(lax.ppermute(late, 'dp', [(d, d ^ stride) for d in range(NDEV)]))
        params, w, m, norm = publish([params, w, m], norm)
        *pieces, norm = lax.optimization_barrier((*pieces, norm))
        others = [lax.ppermute(piece, 'dp', [(d, d ^ 1) for d in range(NDEV)]) for piece in pieces]
        params, v = place_late(params, pieces, False, (v,))
        params, = place_late(params, others, True)
        return params.reshape(-1), w.reshape(-1), m.reshape(-1), v.reshape(-1), norm

    return jax.shard_map(local_step, mesh=mesh, in_specs=(P('dp', None), P('dp'), P('dp'), P('dp'), P('dp'), P()), out_specs=(P(), P('dp'), P('dp'), P('dp'), P()), check_vma=False)
```
